256 devices in a mesh: band: 32 (over y_hi, z, core), fft: 8 (over x, y_lo).
Axes of the slice: x: 4, y: 4 (y_hi: 2, y_lo: 2; y = y_hi * 2 + y_lo), z: 8, core: 2. Of those that a mesh axis runs over, the one named last changes fastest.
Arguments:
- coefficients: float32 [32, 2, 72, 5184], P('band', None, None, 'fft'), may hold values from -0.009765625 to 0.009765625
- col_index: int32 [5184], replicated, may hold values from 0 to 5183, each once
- occupation: int32 [32], P('band'), may hold values from 1 to 4
Outputs:
- density: float32 [288, 288, 288], P('band', 'fft')
The draws below stay inside these ranges and needn't reach their ends.
Inputs may be any that keep to these rules, and one draw needn't show every extreme that they name: `col_index`: each number of the range appears once.
All inputs are finite; a program needn't handle non-finite values.
Results may differ from the reference program's by a relative error of at most 0.0003.
Values sent between devices are 32-bit elements; how exact they have to be, the bound alone decides.
A program may use at most 64 MiB of HBM per device.

```python
import jax
import jax.numpy as jnp
from jax import lax

NC = 144
NF = 288
KZ = 72
R = 36
NCOLS = 5184
BANDS = 32


def set_ends(values, rng, smallest, top_value):
    index_at = [jax.random.randint(jax.random.fold_in(rng, axis), (), 0, length) for axis, length in enumerate(values.shape)]
    widest = values.shape.index(max(values.shape))
    next_to = index_at[:widest] + [(index_at[widest] + 1) % values.shape[widest]] + index_at[widest + 1:]
    return values.at[tuple(index_at)].set(smallest).at[tuple(next_to)].set(top_value)


def block_levels(stream_key, extent, cuts, least, top_value):
    def one(dim, parts):
        steps = jax.random.uniform(jax.random.fold_in(jax.random.fold_in(stream_key, 6), dim), (parts,), jnp.float32, least / len(cuts), top_value / len(cuts))
        return jnp.repeat(jnp.exp(steps), extent[dim] // parts).reshape((-1,) + (1,) * (len(extent) - dim - 1))

    loudness = one(*cuts[0])
    for cut in cuts[1:]:
        loudness = loudness * one(*cut)
    return loudness


def noise(own_key, shape, scale, limit, shards=(), kind=jnp.bfloat16):
    entries = jax.random.normal(own_key, shape, jnp.float32) * scale
    if len(shards) > 0:
        entries = block_levels(own_key, shape, shards, -0.22, 0.18) * entries
    return jnp.clip(entries, min=-limit, max=limit).astype(kind)


def setup_inputs(seed: int = 0) -> dict:
    splits = jax.random.split(jax.random.key(seed), 4)
    return {
        "coefficients": noise(splits[0], (BANDS, 2, KZ, NCOLS), (8 * R**3) ** -0.5, 0.009765625, ((0, 32), (3, 8)), jnp.float32),
        "col_index": jax.random.permutation(splits[1], NCOLS).astype(jnp.int32),
        "occupation": set_ends(jax.random.randint(splits[2], (BANDS,), 1, 5), jax.random.fold_in(splits[2], 1), 1, 4).astype(jnp.int32),
    }


def sphere_mask(radius, side_len):
    wave_index = jnp.arange(side_len, dtype=jnp.int32) - radius
    square = wave_index * wave_index
    total_sq = square[:, None, None] + square[None, :, None] + square[None, None, :]
    return (total_sq <= radius * radius).astype(jnp.float32)


def reference(coefficients, col_index, occupation):
    inverse = jnp.zeros((NCOLS,), jnp.int32).at[col_index].set(jnp.arange(NCOLS, dtype=jnp.int32))
    inside = sphere_mask(R, KZ)

    def add_band(band_index, summed):
        box_grid = jnp.take(coefficients[band_index], inverse, axis=2).reshape(2, KZ, KZ, KZ)
        box_grid = jnp.transpose(box_grid, (0, 2, 3, 1)) * inside
        spectrum = lax.complex(box_grid[0], box_grid[1])
        padded = jnp.zeros((NC, NC, NC), spectrum.dtype).at[:KZ, :KZ, :KZ].set(spectrum)
        padded = jnp.roll(padded, (-R, -R, -R), axis=(0, 1, 2))
        wave_field = jnp.fft.ifftn(padded) * float(NC * NC * NC)
        real_part = jnp.real(wave_field)
        imag_part = jnp.imag(wave_field)
        moduli = real_part * real_part + imag_part * imag_part
        return summed + occupation[band_index].astype(jnp.float32) * moduli

    coarse_density = lax.fori_loop(0, BANDS, add_band, jnp.zeros((NC, NC, NC), jnp.float32)) / BANDS
    spectrum = jnp.fft.fftn(coarse_density) / float(NC * NC * NC)
    kept_mask = (jnp.arange(NC, dtype=jnp.int32) != NC // 2).astype(jnp.float32)
    spectrum = spectrum * (kept_mask[:, None, None] * kept_mask[None, :, None] * kept_mask[None, None, :])
    target = jnp.arange(NC, dtype=jnp.int32)
    target = jnp.where(target < NC // 2, target, target + NF - NC)
    fine_spec = jnp.zeros((NF, NF, NF), spectrum.dtype)
    fine_spec = fine_spec.at[target[:, None, None], target[None, :, None], target[None, None, :]].set(spectrum)
    density = jnp.real(jnp.fft.ifftn(fine_spec)) * float(NF * NF * NF)
    return density.astype(jnp.float32)
```

```python
import functools
import math

import jax
import jax.numpy as jnp
import numpy as np
from jax import lax
from jax.experimental import pallas as pl
from jax.experimental.pallas import tpu as pltpu
from jax.sharding import PartitionSpec as P

NC = 144
NF = 288
KZ = 72
R = 36
NCOLS = 5184
LC = 648
NP = 18
HALF = 1408
BF16 = jnp.bfloat16
F32 = jnp.float32
MESH = pl.DeviceIdType.MESH


def hi_lo(table):
    table = np.asarray(table, np.float64)
    hi = table.astype(np.float32).astype(jnp.bfloat16)
    lo = (table - hi.astype(np.float64)).astype(np.float32).astype(jnp.bfloat16)
    return hi, lo


def phases(points):
    k = np.arange(KZ) - R
    ang = 2.0 * np.pi * ((k[:, None] * np.arange(points)[None, :]) % points) / points
    return np.cos(ang), np.sin(ang)


def interpolation():
    d = np.arange(NF)[:, None] - 2 * np.arange(NC)[None, :]
    k = np.arange(1, NC // 2)
    ang = 2.0 * np.pi * ((d[:, :, None] * k) % NF) / NF
    return (1.0 + 2.0 * np.cos(ang).sum(axis=2)) / NC


def line_table():
    cos, sin = phases(NC)
    w = np.zeros((2, KZ, 8, 128))
    for j in range(8):
        c, s = cos[:, NP * j : NP * j + NP], sin[:, NP * j : NP * j + NP]
        w[0, :, j, :NP] = c
        w[1, :, j, :NP] = -s
        w[0, :, j, NP : 2 * NP] = s
        w[1, :, j, NP : 2 * NP] = c
    return hi_lo(w.reshape(2 * KZ, 1024))


def stacked(table):
    hi, lo = hi_lo(table)
    return np.concatenate([hi, hi, lo], axis=1)


def first_table():
    cos, sin = phases(NC)
    return stacked(np.block([[cos.T, -sin.T], [sin.T, cos.T]]))


def second_tables():
    cos, sin = phases(NC)
    ch, cl = hi_lo(cos)
    sh, sl = hi_lo(sin)
    return ch, cl, sh, sl


def owner_rows():
    m = interpolation()
    rows = np.zeros((8, 5, 8, NC))
    for zc in range(8):
        for y in range(2):
            for c in range(2):
                g = NC * y + 18 * zc + 9 * c
                rows[zc, 2 * y + c] = m[g : g + 8]
                rows[zc, 4, 2 * y + c] = m[g + 8]
    return stacked(rows.reshape(320, NC))


def split(x):
    hi = x.astype(BF16)
    lo = (x - hi.astype(F32)).astype(BF16)
    return hi, lo


def dot(a, b):
    return jnp.dot(a, b, preferred_element_type=F32)


def lines_kernel(coef_ref, radial_ref, wh_ref, wl_ref, out_ref):
    k = lax.broadcasted_iota(jnp.int32, (KZ, LC), 0).astype(F32) - R
    inside = k * k + radial_ref[...] <= float(R * R)
    x = jnp.concatenate(
        [jnp.where(inside, coef_ref[0, 0], 0.0), jnp.where(inside, coef_ref[0, 1], 0.0)], axis=0
    )
    xt = x.T
    hi, lo = split(xt)
    for j in range(8):
        cols = slice(128 * j, 128 * j + 128)
        wh, wl = wh_ref[:, cols], wl_ref[:, cols]
        y = dot(hi, wh) + dot(lo, wh) + dot(hi, wl)
        out_ref[j] = (
            y[0:216] + pltpu.roll(y[216:432], 36, 1) + pltpu.roll(y[432:648], 72, 1)
        )


def lines(coefficients, radial):
    wh, wl = line_table()
    return pl.pallas_call(
        lines_kernel,
        out_shape=jax.ShapeDtypeStruct((8, 216, 128), F32),
        in_specs=[pl.BlockSpec(memory_space=pltpu.VMEM)] * 4,
        out_specs=pl.BlockSpec(memory_space=pltpu.VMEM),
        compiler_params=pltpu.CompilerParams(vmem_limit_bytes=40 * 2**20),
    )(coefficients, radial, jnp.asarray(wh), jnp.asarray(wl))


def planes_kernel(
    recv_ref, cols_ref, occ_ref, ch_ref, cl_ref, sh_ref, sl_ref, t2_ref, m3_ref,
    out_ref, rows_ref, grid_ref, g_ref, hall_ref,
):
    def unpack(s, carry):
        block = recv_ref[s]
        base = s * LC
        rows_ref[pl.ds(base, 216), :] = block
        rows_ref[pl.ds(base + 216, 216), :] = pltpu.roll(block, 128 - 36, 1)
        rows_ref[pl.ds(base + 432, 216), :] = pltpu.roll(block, 128 - 72, 1)
        return carry

    lax.fori_loop(0, 8, unpack, 0)

    def scatter(i, carry):
        for u in range(16):
            n = i * 16 + u
            grid_ref[pl.ds(cols_ref[n], 1), :] = rows_ref[pl.ds(n, 1), :]
        return carry

    lax.fori_loop(0, NCOLS // 16, scatter, 0)

    def turn(k0, carry):
        block = grid_ref[pl.ds(k0 * KZ, 128), :]
        t = block.T
        g_ref[pl.ds(k0, 36, stride=KZ), :] = t[0:36]
        return carry

    lax.fori_loop(0, KZ, turn, 0)

    ch, cl, sh, sl = ch_ref[...], cl_ref[...], sh_ref[...], sl_ref[...]
    for h in range(2):
        hall_ref[:, HALF * h + 9 * NC : HALF * (h + 1)] = jnp.zeros((NC, HALF - 9 * NC), F32)
    for part in range(6):
        rows = 3 * KZ
        re_h, re_l = split(g_ref[rows * part : rows * (part + 1), 0:KZ])
        im_h, im_l = split(g_ref[NP * KZ + rows * part : NP * KZ + rows * (part + 1), 0:KZ])
        half_re = (dot(re_h, ch) + dot(re_l, ch) + dot(re_h, cl)) - (
            dot(im_h, sh) + dot(im_l, sh) + dot(im_h, sl)
        )
        half_im = (dot(re_h, sh) + dot(re_l, sh) + dot(re_h, sl)) + (
            dot(im_h, ch) + dot(im_l, ch) + dot(im_h, cl)
        )
        for u in range(3):
            z = 3 * part + u
            lane = HALF * (z // 9) + NC * (z % 9)
            hall_ref[0:KZ, lane : lane + NC] = half_re[KZ * u : KZ * (u + 1)]
            hall_ref[KZ : 2 * KZ, lane : lane + NC] = half_im[KZ * u : KZ * (u + 1)]

    weight = occ_ref[0].astype(F32) * (1.0 / 32.0)
    for h in range(2):
        for start in range(0, HALF, 256):
            width = min(256, HALF - start)
            lane = slice(HALF * h + start, HALF * h + start + width)
            hh, hl = split(hall_ref[:, lane])
            hst = jnp.concatenate([hh, hl, hh], axis=0)
            psi = dot(t2_ref[...], hst)
            re, im = psi[0:NC], psi[NC : 2 * NC]
            dh, dl = split((re * re + im * im) * weight)
            dst = jnp.concatenate([dh, dl, dh], axis=0)
            s1 = dot(m3_ref[...], dst)
            out_ref[h, :, :, :, start : start + width] = s1.reshape(8, 5, 8, width)


def planes(recv, cols, occ):
    ch, cl, sh, sl = second_tables()
    smem = pl.BlockSpec(memory_space=pltpu.SMEM)
    vmem = pl.BlockSpec(memory_space=pltpu.VMEM)
    return pl.pallas_call(
        planes_kernel,
        out_shape=jax.ShapeDtypeStruct((2, 8, 5, 8, HALF), F32),
        in_specs=[vmem, smem, smem] + [vmem] * 6,
        out_specs=vmem,
        scratch_shapes=[
            pltpu.VMEM((NCOLS, 128), F32),
            pltpu.VMEM((NCOLS + 56, 128), F32),
            pltpu.VMEM((36 * KZ, 128), F32),
            pltpu.VMEM((NC, 2 * HALF), F32),
        ],
        compiler_params=pltpu.CompilerParams(vmem_limit_bytes=56 * 2**20),
    )(recv, cols, occ, *(jnp.asarray(t) for t in (ch, cl, sh, sl, first_table(), owner_rows())))


ALONE = {0: (3, 4), 1: (0, 1, 2)}


def sums_kernel(
    part_ref, mh_ref, ml_ref, out_ref,
    pair, held, sent, acc, other, tot, fin, left, fine, packed, given, got, turned,
    pair_s, pair_r, ring_s, ring_r, other_s, other_r, fin_s, fin_r, got_s, got_r,
):
    band = lax.axis_index("band")
    me = lax.axis_index("fft")
    y, zc, c = band // 16, (band // 2) % 8, band % 2

    def at(yy, zz, cc):
        return {"band": yy * 16 + zz * 2 + cc, "fft": me}

    partner = at(y, zc, 1 - c)
    ring_to = (at(y, (zc + 7) % 8, c), at(y, (zc + 1) % 8, c))
    across = at(1 - y, zc, c)
    peers = [{"band": band, "fft": (me + k) % 8} for k in range(1, 8)]

    barrier = pltpu.get_barrier_semaphore()
    everyone = [partner, *ring_to, across, *peers]
    for device in everyone:
        pl.semaphore_signal(barrier, inc=1, device_id=device, device_id_type=MESH)
    pl.semaphore_wait(barrier, len(everyone))

    def copy(src, dst, send, recv, device):
        made = pltpu.make_async_remote_copy(
            src_ref=src, dst_ref=dst, send_sem=send, recv_sem=recv, device_id=device, device_id_type=MESH
        )
        made.start()
        return made

    started = []
    pairs = {}
    for rel in (4, 5, 3, 6, 2, 7, 1, 0):
        pairs[rel] = copy(
            part_ref.at[1 - c, (zc + rel) % 8], pair.at[rel], pair_s.at[rel], pair_r.at[rel], partner
        )
        started.append(pairs[rel])

    group = (2 * (1 - y), 2 * (1 - y) + 1, 4, 2 * y, 2 * y + 1)
    ready = set()

    def own(rel, lg):
        if rel not in ready:
            pairs[rel].wait_recv()
            ready.add(rel)
        return part_ref[c, (zc + rel) % 8, group[lg]] + pair[rel, group[lg]]

    ring = {}
    for step in range(4):
        away = 4 - step
        for lg in range(5):
            for way in range(2):
                if step == 0 and lg not in ALONE[way]:
                    continue
                rel = (8 - away) % 8 if way == 0 else away
                value = own(rel, lg)
                before = ring.get((way, step - 1, lg))
                if before is not None:
                    before.wait_recv()
                    value = value + held[way, step - 1, lg]
                sent[way, step, lg] = value
                ring[way, step, lg] = copy(
                    sent.at[way, step, lg], held.at[way, step, lg],
                    ring_s.at[way, step, lg], ring_r.at[way, step, lg], ring_to[way],
                )
                started.append(ring[way, step, lg])
    over = []
    for lg in range(5):
        value = own(0, lg)
        for way in range(2):
            ring[way, 3, lg].wait_recv()
            value = value + held[way, 3, lg]
        acc[lg] = value
        if lg < 3:
            over.append(copy(acc.at[lg], other.at[lg], other_s.at[lg], other_r.at[lg], across))
    started += over
    for lg in range(3):
        over[lg].wait_recv()
    tot[0] = acc[3] + other[0]
    tot[1] = acc[4] + other[1]
    tot[2] = acc[2] + other[2]
    last = [
        copy(tot.at[1 - c], fin.at[c, 0], fin_s.at[0], fin_r.at[0], partner),
        copy(tot.at[2], fin.at[c, 1], fin_s.at[1], fin_r.at[1], partner),
    ]
    started += last
    fin[c, 0] = tot[c]
    fin[c, 1] = tot[2]
    for one in last:
        one.wait_recv()

    for h in range(2):
        ninth = fin[h, 1, pl.ds(2 * y + c, 1), :]
        for u in range(9):
            z = 9 * h + u
            left[8 * z : 8 * z + 8, :] = fin[h, 0, :, NC * u : NC * (u + 1)]
            left[NC + z : NC + z + 1, :] = ninth[:, NC * u : NC * (u + 1)]
    lh, ll = split(left[...])
    mh, ml = mh_ref[...], ml_ref[...]
    value = dot(lh, mh) + dot(ll, mh) + dot(lh, ml)
    for t in range(3):
        fine[t, :, 0 : min(128, NF - 128 * t)] = value[:, 128 * t : min(128 * (t + 1), NF)]
    for g in range(9):
        here = pl.ds(g, NP, stride=8) if g < 8 else pl.ds(NC, NP)
        rows = jnp.concatenate([fine[t, here, :] for t in range(3)], axis=1)
        for j in range(8):
            packed[j, 0:NP, 36 * g : 36 * g + 36] = rows[:, 36 * j : 36 * j + 36]
    for j in range(8):
        for t in range(3):
            given[j, NP * t : NP * (t + 1), :] = packed[j, 0:NP, 128 * t : 128 * (t + 1)]
    moves = []
    for k in range(1, 8):
        moves.append(
            copy(given.at[(me + k) % 8], got.at[me], got_s.at[k], got_r.at[k], peers[k - 1])
        )
    started += moves
    got[me] = given[me]
    for one in moves:
        one.wait_recv()
    for j in range(8):
        for t in range(3):
            turned[NP * j : NP * (j + 1), 128 * t : 128 * (t + 1)] = got[j, NP * t : NP * (t + 1), :]
    rh, rl = split(turned[...].T)
    for g in range(9):
        a, b = rh[36 * g : 36 * g + 36], rl[36 * g : 36 * g + 36]
        out_ref[g] = dot(a, mh) + dot(b, mh) + dot(a, ml)
    for one in started:
        one.wait_send()


def sums(part):
    mh, ml = hi_lo(interpolation().T)
    vmem = pl.BlockSpec(memory_space=pltpu.VMEM)
    dma = pltpu.SemaphoreType.DMA
    block = (5, 8, HALF)
    return pl.pallas_call(
        sums_kernel,
        out_shape=jax.ShapeDtypeStruct((9, 36, NF), F32),
        in_specs=[vmem] * 3,
        out_specs=vmem,
        scratch_shapes=[
            pltpu.VMEM((8, *block), F32),
            pltpu.VMEM((2, 4, *block), F32),
            pltpu.VMEM((2, 4, *block), F32),
            pltpu.VMEM(block, F32),
            pltpu.VMEM((3, 8, HALF), F32),
            pltpu.VMEM((3, 8, HALF), F32),
            pltpu.VMEM((2, 2, 8, HALF), F32),
            pltpu.VMEM((168, NC), F32),
            pltpu.VMEM((3, 168, 128), F32),
            pltpu.VMEM((8, 24, 384), F32),
            pltpu.VMEM((8, 56, 128), F32),
            pltpu.VMEM((8, 56, 128), F32),
            pltpu.VMEM((NC, 384), F32),
            dma((8,)), dma((8,)),
            dma((2, 4, 5)), dma((2, 4, 5)),
            dma((3,)), dma((3,)),
            dma((2,)), dma((2,)),
            dma((8,)), dma((8,)),
        ],
        compiler_params=pltpu.CompilerParams(
            collective_id=0, has_side_effects=True, vmem_limit_bytes=40 * 2**20
        ),
    )(part, jnp.asarray(mh), jnp.asarray(ml))


def local(coefficients, col_index, occupation):
    mine = lax.dynamic_slice_in_dim(col_index, lax.axis_index("fft") * LC, LC)
    k0, k1 = mine // KZ - R, mine % KZ - R
    radial = (k0 * k0 + k1 * k1).astype(F32)[None, :]
    packed = lines(coefficients, radial)
    recv = lax.all_to_all(packed, "fft", 0, 0)
    return sums(planes(recv, col_index, occupation))


def solution(mesh):
    return jax.shard_map(
        local,
        mesh=mesh,
        in_specs=(P("band", None, None, "fft"), P(), P("band")),
        out_specs=P("band", "fft", None),
        check_vma=False,
    )
```

```python
import functools
import math

import jax
import jax.numpy as jnp
import numpy as np
from jax import lax
from jax.experimental import pallas as pl
from jax.experimental.pallas import tpu as pltpu
from jax.sharding import PartitionSpec as P

NC = 144
NF = 288
KZ = 72
R = 36
NCOLS = 5184
LC = 648
NP = 18
HALF = 1408
BF16 = jnp.bfloat16
F32 = jnp.float32
MESH = pl.DeviceIdType.MESH


def hi_lo(table):
    table = np.asarray(table, np.float64)
    hi = table.astype(np.float32).astype(jnp.bfloat16)
    lo = (table - hi.astype(np.float64)).astype(np.float32).astype(jnp.bfloat16)
    return hi, lo


def phases(points):
    k = np.arange(KZ) - R
    ang = 2.0 * np.pi * ((k[:, None] * np.arange(points)[None, :]) % points) / points
    return np.cos(ang), np.sin(ang)


def interpolation():
    d = np.arange(NF)[:, None] - 2 * np.arange(NC)[None, :]
    k = np.arange(1, NC // 2)
    ang = 2.0 * np.pi * ((d[:, :, None] * k) % NF) / NF
    return (1.0 + 2.0 * np.cos(ang).sum(axis=2)) / NC


def line_table():
    cos, sin = phases(NC)
    w = np.zeros((2, KZ, 3, 128))
    for d in range(16):
        c, s = cos[:, 9 * d : 9 * d + 9], sin[:, 9 * d : 9 * d + 9]
        t, lane = d // 7, 18 * (d % 7)
        w[0, :, t, lane : lane + 9] = c
        w[1, :, t, lane : lane + 9] = -s
        w[0, :, t, lane + 9 : lane + 18] = s
        w[1, :, t, lane + 9 : lane + 18] = c
    return hi_lo(w.reshape(2 * KZ, 384))


def stacked(table):
    hi, lo = hi_lo(table)
    return np.concatenate([hi, hi, lo], axis=1)


def first_table():
    cos, sin = phases(NC)
    return stacked(np.block([[cos.T, -sin.T], [sin.T, cos.T]]))


def second_tables():
    cos, sin = phases(NC)
    ch, cl = hi_lo(cos)
    sh, sl = hi_lo(sin)
    return ch, cl, sh, sl


def owner_rows():
    m = interpolation()
    rows = np.zeros((8, 5, 8, NC))
    for zc in range(8):
        for y in range(2):
            for c in range(2):
                g = NC * y + 18 * zc + 9 * c
                rows[zc, 2 * y + c] = m[g : g + 8]
                rows[zc, 4, 2 * y + c] = rows[zc, 4, 4 + 2 * y + c] = m[g + 8]
    return stacked(rows.reshape(320, NC))


def split(x):
    hi = x.astype(BF16)
    lo = (x - hi.astype(F32)).astype(BF16)
    return hi, lo


def dot(a, b):
    return jnp.dot(a, b, preferred_element_type=F32)


FAR = ((2, 1), (2, 0), (1, 1), (3, 1), (1, 0), (3, 0), (0, 1), (0, 0))


def lines_kernel(
    coef_hbm, radial_ref, occ_ref, wh_hbm, wl_hbm, out_ref,
    coef, wh, wl, lanes, given, got, load, give_s, got_r,
):
    loads = [
        pltpu.make_async_copy(src, dst, load.at[i])
        for i, (src, dst) in enumerate(((coef_hbm, coef), (wh_hbm, wh), (wl_hbm, wl)))
    ]
    for one in loads:
        one.start()
    band, me = lax.axis_index("band"), lax.axis_index("fft")
    c, x, y = band % 2, me // 2, me % 2
    targets = []
    for dx, dy in FAR:
        for dc in (1, 0):
            if (dx, dy, dc) != (0, 0, 0):
                f, cc = ((x + dx) % 4) * 2 + (y + dy) % 2, (c + dc) % 2
                targets.append((f, cc, {"band": band - c + cc, "fft": f}))
    barrier = pltpu.get_barrier_semaphore()
    for _, _, device in targets:
        pl.semaphore_signal(barrier, inc=1, device_id=device, device_id_type=MESH)

    k = lax.broadcasted_iota(jnp.int32, (KZ, LC), 0).astype(F32) - R
    inside = k * k + radial_ref[...] <= float(R * R)
    scale = jnp.sqrt(jnp.full((1, LC), occ_ref[0].astype(F32) * (1.0 / 32.0)))
    scale = jnp.where(inside, scale, 0.0)
    for one in loads:
        one.wait()
    xt = jnp.concatenate([coef[0, 0] * scale, coef[0, 1] * scale], axis=0).T
    hi, lo = split(xt)
    value = dot(hi, wh[...]) + dot(lo, wh[...]) + dot(hi, wl[...])
    for t in range(3):
        lanes[t] = value[:, 128 * t : 128 * (t + 1)]
    lane = lax.broadcasted_iota(jnp.int32, (96, 128), 1)

    def packed(d):
        t, e = d // 7, d % 7
        tile = lanes.at[t]
        result = pltpu.roll(tile[0:96, :], lax.rem(7 * 128 - 18 * e, 128), 1)
        for q in range(1, 7):
            n = 96 if q < 6 else 72
            turned = pltpu.roll(tile[96 * q : 96 * q + n, :], lax.rem(7 * 128 + 18 * q - 18 * e, 128), 1)
            if n < 96:
                turned = jnp.concatenate([turned, jnp.zeros((96 - n, 128), F32)], axis=0)
            result = jnp.where(lane >= 18 * q, turned, result)
        return result

    moves = []
    for i, (f, cc, device) in enumerate(targets):
        given[i] = packed(2 * f + cc)
        if i == 0:
            pl.semaphore_wait(barrier, len(targets))
        move = pltpu.make_async_remote_copy(
            src_ref=given.at[i], dst_ref=got.at[2 * me + c],
            send_sem=give_s.at[i], recv_sem=got_r.at[i], device_id=device, device_id_type=MESH,
        )
        move.start()
        moves.append(move)
    got[2 * me + c] = packed(2 * me + c)

    def unpack(f):
        base = f * LC
        for q in range(7):
            n = 96 if q < 6 else 72
            first = pltpu.roll(got[2 * f, 0:n, :], (128 - 18 * q) % 128, 1) if q else got[2 * f, 0:n, :]
            second = pltpu.roll(got[2 * f + 1, 0:n, :], (128 + 18 - 18 * q) % 128, 1)
            out_ref[pl.ds(base + 96 * q, n), :] = jnp.where(lane[0:n] < 18, first, second)

    for i in reversed(range(8)):
        dx, dy = FAR[i]
        for move in moves[2 * i : 2 * i + 2]:
            move.wait_recv()
        unpack(((x + 4 - dx) % 4) * 2 + (y + dy) % 2)
    for move in moves:
        move.wait_send()


def lines(coefficients, radial, occ):
    wh, wl = line_table()
    vmem = pl.BlockSpec(memory_space=pltpu.VMEM)
    hbm = pl.BlockSpec(memory_space=pltpu.HBM)
    dma = pltpu.SemaphoreType.DMA
    return pl.pallas_call(
        lines_kernel,
        out_shape=jax.ShapeDtypeStruct((NCOLS, 128), F32),
        in_specs=[hbm, vmem, pl.BlockSpec(memory_space=pltpu.SMEM), hbm, hbm],
        out_specs=vmem,
        scratch_shapes=[
            pltpu.VMEM((1, 2, KZ, LC), F32),
            pltpu.VMEM((2 * KZ, 384), BF16),
            pltpu.VMEM((2 * KZ, 384), BF16),
            pltpu.VMEM((3, LC, 128), F32),
            pltpu.VMEM((15, 96, 128), F32),
            pltpu.VMEM((16, 96, 128), F32),
            dma((3,)), dma((15,)), dma((15,)),
        ],
        compiler_params=pltpu.CompilerParams(
            collective_id=1, has_side_effects=True, vmem_limit_bytes=24 * 2**20
        ),
    )(coefficients, radial, occ, jnp.asarray(wh), jnp.asarray(wl))


def planes_kernel(
    rows_ref, cols_ref, ch_ref, cl_ref, sh_ref, sl_ref, t2_ref, m3_ref,
    out_ref, grid_ref, g_ref, hall_ref,
):
    def scatter(i, carry):
        for u in range(16):
            n = i * 16 + u
            grid_ref[pl.ds(cols_ref[n], 1), :] = rows_ref[pl.ds(n, 1), :]
        return carry

    lax.fori_loop(0, NCOLS // 16, scatter, 0)

    def turn(i, carry):
        for u in range(8):
            k0 = i * 8 + u
            t = grid_ref[pl.ds(k0 * KZ, 128), :].T
            g_ref[pl.ds(k0, 36, stride=KZ), :] = t[0:36]
        return carry

    lax.fori_loop(0, KZ // 8, turn, 0)

    ch, cl, sh, sl = ch_ref[...], cl_ref[...], sh_ref[...], sl_ref[...]
    for h in range(2):
        hall_ref[:, HALF * h + 9 * NC : HALF * (h + 1)] = jnp.zeros((NC, HALF - 9 * NC), F32)
    for part in range(6):
        h, first = part // 3, 3 * (part % 3)
        rows = 3 * KZ
        base = (18 * h + first) * KZ
        re_h, re_l = split(g_ref[base : base + rows, 0:KZ])
        base += 9 * KZ
        im_h, im_l = split(g_ref[base : base + rows, 0:KZ])
        half_re = (dot(re_h, ch) + dot(re_l, ch) + dot(re_h, cl)) - (
            dot(im_h, sh) + dot(im_l, sh) + dot(im_h, sl)
        )
        half_im = (dot(re_h, sh) + dot(re_l, sh) + dot(re_h, sl)) + (
            dot(im_h, ch) + dot(im_l, ch) + dot(im_h, cl)
        )
        for u in range(3):
            at = HALF * h + NC * (first + u)
            hall_ref[0:KZ, at : at + NC] = half_re[KZ * u : KZ * (u + 1)]
            hall_ref[KZ : 2 * KZ, at : at + NC] = half_im[KZ * u : KZ * (u + 1)]

    def interpolated(tiles):
        total = 0.0
        for h in range(2):
            field = [hall_ref[:, HALF * h + 128 * t : HALF * h + 128 * (t + 1)] for t in tiles]
            hh, hl = split(jnp.concatenate(field, axis=1))
            psi = dot(t2_ref[...], jnp.concatenate([hh, hl, hh], axis=0))
            re, im = psi[0:NC], psi[NC : 2 * NC]
            total = total + re * re + im * im
        dh, dl = split(total)
        return dot(m3_ref[...], jnp.concatenate([dh, dl, dh], axis=0))

    row = lax.broadcasted_iota(jnp.int32, (8, 128), 0)
    lane = lax.broadcasted_iota(jnp.int32, (8, 128), 1)
    for t in range(5):
        both = interpolated((t, t + 5))
        left, right = both[:, 0:128].reshape(8, 5, 8, 128), both[:, 128:256].reshape(8, 5, 8, 128)
        for p in range(4):
            out_ref[:, 10 * p + t] = left[:, p]
            out_ref[:, 10 * p + t + 5] = right[:, p]
        out_ref[:, 40 + t] = jnp.where(row[None] < 4, left[:, 4], right[:, 4])
    rest = interpolated((10,)).reshape(8, 5, 8, 128)
    for zc in range(8):
        value = rest[zc, 0]
        for p in range(1, 5):
            value = jnp.where(lane >= 16 * p, pltpu.roll(rest[zc, p], 16 * p, 1), value)
        out_ref[zc, 45] = value


def planes(rows, cols):
    ch, cl, sh, sl = second_tables()
    smem = pl.BlockSpec(memory_space=pltpu.SMEM)
    vmem = pl.BlockSpec(memory_space=pltpu.VMEM)
    return pl.pallas_call(
        planes_kernel,
        out_shape=jax.ShapeDtypeStruct((8, 46, 8, 128), F32),
        in_specs=[vmem, smem] + [vmem] * 6,
        out_specs=vmem,
        scratch_shapes=[
            pltpu.VMEM((NCOLS + 56, 128), F32),
            pltpu.VMEM((36 * KZ, 128), F32),
            pltpu.VMEM((NC, 2 * HALF), F32),
        ],
        compiler_params=pltpu.CompilerParams(vmem_limit_bytes=32 * 2**20),
    )(rows, cols, *(jnp.asarray(t) for t in (ch, cl, sh, sl, first_table(), owner_rows())))


ALONE = {0: (3, 4), 1: (0, 1, 2)}


def sums_kernel(
    part_ref, mh_ref, ml_ref, out_ref,
    held, sent, acc, other, tot, fin, left, fine, packed, given, got, turned,
    ring_s, ring_r, other_s, other_r, fin_s, fin_r, got_s, got_r,
):
    band = lax.axis_index("band")
    me = lax.axis_index("fft")
    y, zc, c = band // 16, (band // 2) % 8, band % 2

    def at(yy, zz, cc):
        return {"band": yy * 16 + zz * 2 + cc, "fft": me}

    partner = at(y, zc, 1 - c)
    ring_to = (at(y, (zc + 7) % 8, c), at(y, (zc + 1) % 8, c))
    across = at(1 - y, zc, c)
    peers = [{"band": band, "fft": (me + k) % 8} for k in range(1, 8)]

    barrier = pltpu.get_barrier_semaphore()
    everyone = [partner, *ring_to, across, *peers]
    for device in everyone:
        pl.semaphore_signal(barrier, inc=1, device_id=device, device_id_type=MESH)
    pl.semaphore_wait(barrier, len(everyone))

    def copy(src, dst, send, recv, device):
        made = pltpu.make_async_remote_copy(
            src_ref=src, dst_ref=dst, send_sem=send, recv_sem=recv, device_id=device, device_id_type=MESH
        )
        made.start()
        return made

    started = []
    theirs, mine = 20 * (1 - y), 20 * y
    group = (pl.ds(theirs, 10), pl.ds(theirs + 10, 10), pl.ds(40, 6), pl.ds(mine, 10), pl.ds(mine + 10, 10))

    ring = {}
    for step in range(4):
        away = 4 - step
        for lg in range(5):
            for way in range(2):
                if step == 0 and lg not in ALONE[way]:
                    continue
                owner = (zc + (8 - away if way == 0 else away)) % 8
                before = ring.get((way, step - 1, lg))
                if before is None:
                    src = part_ref.at[owner, group[lg]]
                else:
                    before.wait_recv()
                    sent[way, step, group[lg]] = part_ref[owner, group[lg]] + held[way, step - 1, group[lg]]
                    src = sent.at[way, step, group[lg]]
                ring[way, step, lg] = copy(
                    src, held.at[way, step, group[lg]],
                    ring_s.at[way, step, lg], ring_r.at[way, step, lg], ring_to[way],
                )
                started.append(ring[way, step, lg])
    over = []
    for lg in range(5):
        for way in range(2):
            ring[way, 3, lg].wait_recv()
        acc[group[lg]] = part_ref[zc, group[lg]] + held[0, 3, group[lg]] + held[1, 3, group[lg]]
        if lg < 3:
            there = (pl.ds(0, 10), pl.ds(10, 10), pl.ds(20, 6))[lg]
            over.append(copy(acc.at[group[lg]], other.at[there], other_s.at[lg], other_r.at[lg], across))
    started += over
    for one in over:
        one.wait_recv()
    tot[pl.ds(0, 10)] = acc[pl.ds(mine, 10)] + other[pl.ds(0, 10)]
    tot[pl.ds(10, 10)] = acc[pl.ds(mine + 10, 10)] + other[pl.ds(10, 10)]
    tot[pl.ds(20, 6)] = acc[pl.ds(40, 6)] + other[pl.ds(20, 6)]
    last = [
        copy(tot.at[pl.ds(10 * (1 - c), 10)], fin.at[c, pl.ds(0, 10)], fin_s.at[0], fin_r.at[0], partner),
        copy(tot.at[pl.ds(20, 6)], fin.at[c, pl.ds(10, 6)], fin_s.at[1], fin_r.at[1], partner),
    ]
    started += last
    fin[c, pl.ds(0, 10)] = tot[pl.ds(10 * c, 10)]
    fin[c, pl.ds(10, 6)] = tot[pl.ds(20, 6)]
    for one in last:
        one.wait_recv()

    which = 2 * y + c
    for h in range(2):
        tail = pltpu.roll(fin[h, 15], lax.rem(128 - 16 * which, 128), 1)
        main = jnp.concatenate([fin[h, t] for t in range(10)] + [tail], axis=1)
        tail = pltpu.roll(fin[h, 15, pl.ds(which, 1), :], 64, 1)
        ninth = jnp.concatenate(
            [fin[h, 10 + t, pl.ds(which, 1), :] for t in range(5)]
            + [fin[h, 10 + t, pl.ds(4 + which, 1), :] for t in range(5)]
            + [tail],
            axis=1,
        )
        for u in range(9):
            z = 9 * h + u
            left[8 * z : 8 * z + 8, :] = main[:, NC * u : NC * (u + 1)]
            left[NC + z : NC + z + 1, :] = ninth[:, NC * u : NC * (u + 1)]
    lh, ll = split(left[...])
    mh, ml = mh_ref[...], ml_ref[...]
    value = dot(lh, mh) + dot(ll, mh) + dot(lh, ml)
    for t in range(3):
        fine[t, :, 0 : min(128, NF - 128 * t)] = value[:, 128 * t : min(128 * (t + 1), NF)]
    for g in range(9):
        here = pl.ds(g, NP, stride=8) if g < 8 else pl.ds(NC, NP)
        rows = jnp.concatenate([fine[t, here, :] for t in range(3)], axis=1)
        for j in range(8):
            packed[j, 0:NP, 36 * g : 36 * g + 36] = rows[:, 36 * j : 36 * j + 36]
    for j in range(8):
        for t in range(3):
            given[j, NP * t : NP * (t + 1), :] = packed[j, 0:NP, 128 * t : 128 * (t + 1)]
    moves = []
    for k in range(1, 8):
        moves.append(
            copy(given.at[(me + k) % 8], got.at[me], got_s.at[k], got_r.at[k], peers[k - 1])
        )
    started += moves
    got[me] = given[me]
    for one in moves:
        one.wait_recv()
    for j in range(8):
        for t in range(3):
            turned[NP * j : NP * (j + 1), 128 * t : 128 * (t + 1)] = got[j, NP * t : NP * (t + 1), :]
    rh, rl = split(turned[...].T)
    for g in range(9):
        a, b = rh[36 * g : 36 * g + 36], rl[36 * g : 36 * g + 36]
        out_ref[g] = dot(a, mh) + dot(b, mh) + dot(a, ml)
    for one in started:
        one.wait_send()


def sums(part):
    mh, ml = hi_lo(interpolation().T)
    vmem = pl.BlockSpec(memory_space=pltpu.VMEM)
    dma = pltpu.SemaphoreType.DMA
    return pl.pallas_call(
        sums_kernel,
        out_shape=jax.ShapeDtypeStruct((9, 36, NF), F32),
        in_specs=[vmem] * 3,
        out_specs=vmem,
        scratch_shapes=[
            pltpu.VMEM((2, 4, 46, 8, 128), F32),
            pltpu.VMEM((2, 4, 46, 8, 128), F32),
            pltpu.VMEM((46, 8, 128), F32),
            pltpu.VMEM((26, 8, 128), F32),
            pltpu.VMEM((26, 8, 128), F32),
            pltpu.VMEM((2, 16, 8, 128), F32),
            pltpu.VMEM((168, NC), F32),
            pltpu.VMEM((3, 168, 128), F32),
            pltpu.VMEM((8, 24, 384), F32),
            pltpu.VMEM((8, 56, 128), F32),
            pltpu.VMEM((8, 56, 128), F32),
            pltpu.VMEM((NC, 384), F32),
            dma((2, 4, 5)), dma((2, 4, 5)),
            dma((3,)), dma((3,)),
            dma((2,)), dma((2,)),
            dma((8,)), dma((8,)),
        ],
        compiler_params=pltpu.CompilerParams(
            collective_id=0, has_side_effects=True, vmem_limit_bytes=24 * 2**20
        ),
    )(part, jnp.asarray(mh), jnp.asarray(ml))


def local(coefficients, col_index, occupation):
    mine = lax.dynamic_slice_in_dim(col_index, lax.axis_index("fft") * LC, LC)
    k0, k1 = mine // KZ - R, mine % KZ - R
    radial = (k0 * k0 + k1 * k1).astype(F32)[None, :]
    rows = lines(coefficients, radial, occupation)
    return sums(planes(rows, col_index))


def solution(mesh):
    return jax.shard_map(
        local,
        mesh=mesh,
        in_specs=(P("band", None, None, "fft"), P(), P("band")),
        out_specs=P("band", "fft", None),
        check_vma=False,
    )
```

```python
import functools
import math

import jax
import jax.numpy as jnp
import numpy as np
from jax import lax
from jax.experimental import pallas as pl
from jax.experimental.pallas import tpu as pltpu
from jax.sharding import PartitionSpec as P

NC = 144
NF = 288
KZ = 72
R = 36
NCOLS = 5184
LC = 648
NP = 18
HALF = 768
FIRST = (0, 5, 9, 14)
COUNT = (5, 4, 5, 4)
BF16 = jnp.bfloat16
F32 = jnp.float32
MESH = pl.DeviceIdType.MESH


def hi_lo(table):
    table = np.asarray(table, np.float64)
    hi = table.astype(np.float32).astype(jnp.bfloat16)
    lo = (table - hi.astype(np.float64)).astype(np.float32).astype(jnp.bfloat16)
    return hi, lo


def phases(points):
    k = np.arange(KZ) - R
    ang = 2.0 * np.pi * ((k[:, None] * np.arange(points)[None, :]) % points) / points
    return np.cos(ang), np.sin(ang)


def interpolation():
    d = np.arange(NF)[:, None] - 2 * np.arange(NC)[None, :]
    k = np.arange(1, NC // 2)
    ang = 2.0 * np.pi * ((d[:, :, None] * k) % NF) / NF
    return (1.0 + 2.0 * np.cos(ang).sum(axis=2)) / NC


def line_table():
    cos, sin = phases(NC)
    w = np.zeros((2, KZ, 3, 128))
    for d in range(32):
        n, z = COUNT[d % 4], NP * (d // 4) + FIRST[d % 4]
        c, s = cos[:, z : z + n], sin[:, z : z + n]
        t, lane = d // 12, 10 * (d % 12)
        w[0, :, t, lane : lane + n] = c
        w[1, :, t, lane : lane + n] = -s
        w[0, :, t, lane + 5 : lane + 5 + n] = s
        w[1, :, t, lane + 5 : lane + 5 + n] = c
    return hi_lo(w.reshape(2 * KZ, 384))


def stacked(table):
    hi, lo = hi_lo(table)
    return np.concatenate([hi, hi, lo], axis=1)


def first_table():
    cos, sin = phases(NC)
    return stacked(np.block([[cos.T, -sin.T], [sin.T, cos.T]]))


def second_tables():
    cos, sin = phases(NC)
    ch, cl = hi_lo(cos)
    sh, sl = hi_lo(sin)
    return ch, cl, sh, sl


def owner_rows():
    m = interpolation()
    rows = np.zeros((8, 5, 8, NC))
    for zc in range(8):
        for y in range(2):
            for c in range(2):
                g = NC * y + 18 * zc + 9 * c
                rows[zc, 2 * y + c] = m[g : g + 8]
                rows[zc, 4, 2 * y + c] = rows[zc, 4, 4 + 2 * y + c] = m[g + 8]
    return stacked(rows.reshape(320, NC))


def split(x):
    hi = x.astype(BF16)
    lo = (x - hi.astype(F32)).astype(BF16)
    return hi, lo


def dot(a, b):
    return jnp.dot(a, b, preferred_element_type=F32)


CHIPS = sorted(
    ((dx, dy) for dx in range(4) for dy in range(4)),
    key=lambda d: (-min(d[0], 4 - d[0]) - min(d[1], 4 - d[1]), d),
)
TARGETS = [(dx, dy, dc) for dx, dy in CHIPS for dc in (1, 0) if (dx, dy, dc) != (0, 0, 0)]


def load_tables(pairs, sems):
    loads = [pltpu.make_async_copy(src, dst, sems.at[i]) for i, (src, dst) in enumerate(pairs)]
    for one in loads:
        one.start()
    return loads


def lines_kernel(
    coef_hbm, cols_hbm, occ_ref, wh_hbm, wl_hbm, out_ref,
    coef, cols, wh, wl, lanes, given, got, load, give_s, got_r,
):
    loads = load_tables(((cols_hbm, cols), (coef_hbm, coef), (wh_hbm, wh), (wl_hbm, wl)), load)
    band, me = lax.axis_index("band"), lax.axis_index("fft")
    yh, zc, c = band // 16, (band // 2) % 8, band % 2
    x, y = me // 2, 2 * yh + me % 2
    slot = 4 * me + 2 * yh + c

    def device(xx, yy, cc):
        return {"band": (yy // 2) * 16 + zc * 2 + cc, "fft": 2 * xx + yy % 2}

    targets = [((x + dx) % 4, (y + dy) % 4, (c + dc) % 2) for dx, dy, dc in TARGETS]
    barrier = pltpu.get_barrier_semaphore()
    for target in targets:
        pl.semaphore_signal(barrier, inc=1, device_id=device(*target), device_id_type=MESH)

    loads[0].wait()
    window = cols[:, pl.ds(pl.multiple_of(640 * me, 128), 704)]
    window = jnp.concatenate([window, window[:, 0:64]], axis=1)
    box = pltpu.roll(window, lax.rem(768 - 8 * me, 768), 1)[:, 0:LC].astype(F32)
    k0 = jnp.floor((box + 0.5) * (1.0 / KZ))
    k1 = box - KZ * k0 - R
    k0 = k0 - R
    k = lax.broadcasted_iota(jnp.int32, (KZ, LC), 0).astype(F32) - R
    inside = k * k + (k0 * k0 + k1 * k1) <= float(R * R)
    scale = jnp.sqrt(jnp.full((1, LC), occ_ref[0].astype(F32) * (1.0 / 32.0)))
    scale = jnp.where(inside, scale, 0.0)
    for one in loads[1:]:
        one.wait()
    xt = jnp.concatenate([coef[0, 0] * scale, coef[0, 1] * scale], axis=0).T
    hi, lo = split(xt)
    value = dot(hi, wh[...]) + dot(lo, wh[...]) + dot(hi, wl[...])
    for t in range(3):
        lanes[t] = value[:, 128 * t : 128 * (t + 1)]
    lane = lax.broadcasted_iota(jnp.int32, (56, 128), 1)
    pieces = [(q, 56 if q < 11 else 32) for q in range(12)]

    def packed(d):
        t, e = d // 12, d % 12
        tile = lanes.at[t]
        result = None
        for q, n in pieces:
            turned = pltpu.roll(tile[56 * q : 56 * q + n, :], lax.rem(10 * 128 + 10 * q - 10 * e, 128), 1)
            if n < 56:
                turned = jnp.concatenate([turned, jnp.zeros((56 - n, 128), F32)], axis=0)
            result = turned if result is None else jnp.where(lane >= 10 * q, turned, result)
        return result

    moves = {}
    for i, target in enumerate(targets):
        xx, yy, cc = target
        given[i] = packed(4 * (2 * xx + yy % 2) + 2 * (yy // 2) + cc)
        if i == 0:
            pl.semaphore_wait(barrier, len(targets))
        move = pltpu.make_async_remote_copy(
            src_ref=given.at[i], dst_ref=got.at[slot],
            send_sem=give_s.at[i], recv_sem=got_r.at[i], device_id=device(*target), device_id_type=MESH,
        )
        move.start()
        moves[TARGETS[i]] = move
    got[slot] = packed(slot)

    def unpack(f):
        base = pl.multiple_of(f * LC, 8)
        for q, n in pieces:
            result = None
            for i in range(4):
                block = got[4 * f + i, 0:n, :]
                shift = (10 * i - 10 * q) % 128
                block = pltpu.roll(block, shift, 1) if shift else block
                result = block if i == 0 else jnp.where(lane[0:n] >= 10 * i, block, result)
            out_ref[pl.ds(base + 56 * q, n), :] = result

    for dx, odd in ((0, 1), (0, 0), (1, 1), (3, 1), (1, 0), (3, 0), (2, 1), (2, 0)):
        for dy in (odd, odd + 2):
            for dc in (0, 1):
                if (dx, dy, dc) in moves:
                    moves[dx, dy, dc].wait_recv()
        unpack(((x + 4 - dx) % 4) * 2 + (y + odd) % 2)
    for move in moves.values():
        move.wait_send()


def lines(coefficients, cols, occ):
    wh, wl = line_table()
    hbm = pl.BlockSpec(memory_space=pltpu.HBM)
    dma = pltpu.SemaphoreType.DMA
    n = len(TARGETS)
    return pl.pallas_call(
        lines_kernel,
        out_shape=jax.ShapeDtypeStruct((NCOLS, 128), F32),
        in_specs=[hbm, hbm, pl.BlockSpec(memory_space=pltpu.SMEM), hbm, hbm],
        out_specs=pl.BlockSpec(memory_space=pltpu.VMEM),
        scratch_shapes=[
            pltpu.VMEM((1, 2, KZ, LC), F32),
            pltpu.VMEM((1, NCOLS), jnp.int32),
            pltpu.VMEM((2 * KZ, 384), BF16),
            pltpu.VMEM((2 * KZ, 384), BF16),
            pltpu.VMEM((3, LC, 128), F32),
            pltpu.VMEM((n, 56, 128), F32),
            pltpu.VMEM((32, 56, 128), F32),
            dma((4,)), dma((n,)), dma((n,)),
        ],
        compiler_params=pltpu.CompilerParams(
            collective_id=1, has_side_effects=True, vmem_limit_bytes=24 * 2**20
        ),
    )(coefficients, cols, occ, jnp.asarray(wh), jnp.asarray(wl))


def planes_kernel(
    rows_ref, cols_ref, ch_hbm, cl_hbm, sh_hbm, sl_hbm, t2_hbm, m3_hbm,
    out_ref, grid_ref, g_ref, hall_ref, ch_ref, cl_ref, sh_ref, sl_ref, t2_ref, m3_ref, load,
):
    loads = load_tables(
        (
            (ch_hbm, ch_ref), (cl_hbm, cl_ref), (sh_hbm, sh_ref),
            (sl_hbm, sl_ref), (t2_hbm, t2_ref), (m3_hbm, m3_ref),
        ),
        load,
    )

    def scatter(i, carry):
        for u in range(16):
            n = i * 16 + u
            grid_ref[pl.ds(cols_ref[n], 1), :] = rows_ref[pl.ds(n, 1), :]
        return carry

    lax.fori_loop(0, NCOLS // 16, scatter, 0)

    def turn(i, carry):
        for u in range(8):
            k0 = i * 8 + u
            t = grid_ref[pl.ds(pl.multiple_of(k0 * KZ, 8), 128), :].T
            g_ref[pl.ds(k0, 40, stride=KZ), :] = t[0:40]
        return carry

    lax.fori_loop(0, KZ // 8, turn, 0)

    for one in loads:
        one.wait()
    ch, cl, sh, sl = ch_ref[...], cl_ref[...], sh_ref[...], sl_ref[...]
    rows = 5 * KZ
    for h in range(4):
        hall_ref[:, HALF * h + 5 * NC : HALF * (h + 1)] = jnp.zeros((NC, HALF - 5 * NC), F32)
        base = 10 * h * KZ
        re_h, re_l = split(g_ref[base : base + rows, 0:KZ])
        im_h, im_l = split(g_ref[base + rows : base + 2 * rows, 0:KZ])
        half_re = (dot(re_h, ch) + dot(re_l, ch) + dot(re_h, cl)) - (
            dot(im_h, sh) + dot(im_l, sh) + dot(im_h, sl)
        )
        half_im = (dot(re_h, sh) + dot(re_l, sh) + dot(re_h, sl)) + (
            dot(im_h, ch) + dot(im_l, ch) + dot(im_h, cl)
        )
        for u in range(5):
            at = HALF * h + NC * u
            hall_ref[0:KZ, at : at + NC] = half_re[KZ * u : KZ * (u + 1)]
            hall_ref[KZ : 2 * KZ, at : at + NC] = half_im[KZ * u : KZ * (u + 1)]

    row = lax.broadcasted_iota(jnp.int32, (8, 128), 0)
    for t in range(3):
        total = 0.0
        for h in range(4):
            field = [hall_ref[:, HALF * h + 128 * i : HALF * h + 128 * (i + 1)] for i in (t, t + 3)]
            hh, hl = split(jnp.concatenate(field, axis=1))
            psi = dot(t2_ref[...], jnp.concatenate([hh, hl, hh], axis=0))
            re, im = psi[0:NC], psi[NC : 2 * NC]
            total = total + (re * re + im * im)
        dh, dl = split(total)
        both = dot(m3_ref[...], jnp.concatenate([dh, dl, dh], axis=0))
        left, right = both[:, 0:128].reshape(8, 5, 8, 128), both[:, 128:256].reshape(8, 5, 8, 128)
        for p in range(4):
            out_ref[:, 6 * p + t] = left[:, p]
            out_ref[:, 6 * p + t + 3] = right[:, p]
        out_ref[:, 24 + t] = jnp.where(row[None] < 4, left[:, 4], right[:, 4])


def planes(rows, cols):
    ch, cl, sh, sl = second_tables()
    tables = (ch, cl, sh, sl, first_table(), owner_rows())
    vmem = pl.BlockSpec(memory_space=pltpu.VMEM)
    return pl.pallas_call(
        planes_kernel,
        out_shape=jax.ShapeDtypeStruct((8, 27, 8, 128), F32),
        in_specs=[vmem, pl.BlockSpec(memory_space=pltpu.SMEM)] + [pl.BlockSpec(memory_space=pltpu.HBM)] * 6,
        out_specs=vmem,
        scratch_shapes=[
            pltpu.VMEM((NCOLS + 56, 128), F32),
            pltpu.VMEM((40 * KZ, 128), F32),
            pltpu.VMEM((NC, 4 * HALF), F32),
            *(pltpu.VMEM(t.shape, BF16) for t in tables),
            pltpu.SemaphoreType.DMA((6,)),
        ],
        compiler_params=pltpu.CompilerParams(vmem_limit_bytes=32 * 2**20),
    )(rows, cols, *(jnp.asarray(t) for t in tables))


ALONE = {0: (0, 1, 2), 1: (3, 4)}


def sums_kernel(
    part_ref, mh_hbm, ml_hbm, out_ref,
    held, sent, acc, fin, left, fine, packed, given, got, turned, mh_ref, ml_ref,
    load, ring_s, ring_r, quad_s, quad_r, got_s, got_r,
):
    loads = load_tables(((mh_hbm, mh_ref), (ml_hbm, ml_ref)), load)
    band = lax.axis_index("band")
    me = lax.axis_index("fft")
    y, zc, c = band // 16, (band // 2) % 8, band % 2
    quarter = 2 * y + c

    def at(yy, zz, cc):
        return {"band": yy * 16 + zz * 2 + cc, "fft": me}

    ring_to = (at(y, (zc + 7) % 8, c), at(y, (zc + 1) % 8, c))
    others = ((1 - y, c), (1 - y, 1 - c), (y, 1 - c))
    quad = [at(yy, zc, cc) for yy, cc in others]
    peers = [{"band": band, "fft": (me + k) % 8} for k in range(1, 8)]

    barrier = pltpu.get_barrier_semaphore()
    everyone = [*ring_to, *quad, *peers]
    for device in everyone:
        pl.semaphore_signal(barrier, inc=1, device_id=device, device_id_type=MESH)
    pl.semaphore_wait(barrier, len(everyone))

    def copy(src, dst, send, recv, device):
        made = pltpu.make_async_remote_copy(
            src_ref=src, dst_ref=dst, send_sem=send, recv_sem=recv, device_id=device, device_id_type=MESH
        )
        made.start()
        return made

    started = []
    group = (
        pl.ds(24, 3),
        *(pl.ds(6 * (2 * yy + cc), 6) for yy, cc in others),
        pl.ds(6 * quarter, 6),
    )

    ring = {}
    for step in range(4):
        away = 4 - step
        for lg in range(5):
            for way in range(2):
                if step == 0 and lg not in ALONE[way]:
                    continue
                owner = (zc + (8 - away if way == 0 else away)) % 8
                before = ring.get((way, step - 1, lg))
                if before is None:
                    src = part_ref.at[owner, group[lg]]
                else:
                    before.wait_recv()
                    sent[way, step, group[lg]] = part_ref[owner, group[lg]] + held[way, step - 1, group[lg]]
                    src = sent.at[way, step, group[lg]]
                ring[way, step, lg] = copy(
                    src, held.at[way, step, group[lg]],
                    ring_s.at[way, step, lg], ring_r.at[way, step, lg], ring_to[way],
                )
                started.append(ring[way, step, lg])
    over = []
    for lg in range(5):
        for way in range(2):
            ring[way, 3, lg].wait_recv()
        acc[group[lg]] = part_ref[zc, group[lg]] + held[0, 3, group[lg]] + held[1, 3, group[lg]]
        for i in range(3):
            if lg == 0:
                there = fin.at[quarter, pl.ds(6, 3)]
            elif lg == i + 1:
                there = fin.at[quarter, pl.ds(0, 6)]
            else:
                continue
            k = 2 * i + (lg > 0)
            over.append(copy(acc.at[group[lg]], there, quad_s.at[k], quad_r.at[k], quad[i]))
    started += over
    fin[quarter, pl.ds(0, 6)] = acc[group[4]]
    fin[quarter, pl.ds(6, 3)] = acc[group[0]]
    for one in over:
        one.wait_recv()

    for s in range(4):
        main = jnp.concatenate([fin[s, t] for t in range(6)], axis=1)
        ninth = jnp.concatenate(
            [fin[s, 6 + t, pl.ds(quarter, 1), :] for t in range(3)]
            + [fin[s, 6 + t, pl.ds(4 + quarter, 1), :] for t in range(3)],
            axis=1,
        )
        for u in range(COUNT[s]):
            z = FIRST[s] + u
            left[8 * z : 8 * z + 8, :] = main[:, NC * u : NC * (u + 1)]
            left[NC + z : NC + z + 1, :] = ninth[:, NC * u : NC * (u + 1)]
    for one in loads:
        one.wait()
    lh, ll = split(left[...])
    mh, ml = mh_ref[...], ml_ref[...]
    value = dot(lh, mh) + dot(ll, mh) + dot(lh, ml)
    for t in range(3):
        fine[t, :, 0 : min(128, NF - 128 * t)] = value[:, 128 * t : min(128 * (t + 1), NF)]
    for g in range(9):
        here = pl.ds(g, NP, stride=8) if g < 8 else pl.ds(NC, NP)
        rows = jnp.concatenate([fine[t, here, :] for t in range(3)], axis=1)
        for j in range(8):
            packed[j, 0:NP, 36 * g : 36 * g + 36] = rows[:, 36 * j : 36 * j + 36]
    for j in range(8):
        for t in range(3):
            given[j, NP * t : NP * (t + 1), :] = packed[j, 0:NP, 128 * t : 128 * (t + 1)]
    moves = []
    for k in range(1, 8):
        moves.append(
            copy(given.at[(me + k) % 8], got.at[me], got_s.at[k], got_r.at[k], peers[k - 1])
        )
    started += moves
    got[me] = given[me]
    for one in moves:
        one.wait_recv()
    for j in range(8):
        for t in range(3):
            turned[NP * j : NP * (j + 1), 128 * t : 128 * (t + 1)] = got[j, NP * t : NP * (t + 1), :]
    rh, rl = split(turned[...].T)
    for g in range(9):
        a, b = rh[36 * g : 36 * g + 36], rl[36 * g : 36 * g + 36]
        out_ref[g] = dot(a, mh) + dot(b, mh) + dot(a, ml)
    for one in started:
        one.wait_send()


def sums(part):
    mh, ml = hi_lo(interpolation().T)
    vmem = pl.BlockSpec(memory_space=pltpu.VMEM)
    dma = pltpu.SemaphoreType.DMA
    return pl.pallas_call(
        sums_kernel,
        out_shape=jax.ShapeDtypeStruct((9, 36, NF), F32),
        in_specs=[vmem] + [pl.BlockSpec(memory_space=pltpu.HBM)] * 2,
        out_specs=vmem,
        scratch_shapes=[
            pltpu.VMEM((2, 4, 27, 8, 128), F32),
            pltpu.VMEM((2, 4, 27, 8, 128), F32),
            pltpu.VMEM((27, 8, 128), F32),
            pltpu.VMEM((4, 9, 8, 128), F32),
            pltpu.VMEM((168, NC), F32),
            pltpu.VMEM((3, 168, 128), F32),
            pltpu.VMEM((8, 24, 384), F32),
            pltpu.VMEM((8, 56, 128), F32),
            pltpu.VMEM((8, 56, 128), F32),
            pltpu.VMEM((NC, 384), F32),
            pltpu.VMEM((NC, NF), BF16),
            pltpu.VMEM((NC, NF), BF16),
            dma((2,)),
            dma((2, 4, 5)), dma((2, 4, 5)),
            dma((6,)), dma((6,)),
            dma((8,)), dma((8,)),
        ],
        compiler_params=pltpu.CompilerParams(
            collective_id=0, has_side_effects=True, vmem_limit_bytes=24 * 2**20
        ),
    )(part, jnp.asarray(mh), jnp.asarray(ml))


def local(coefficients, col_index, occupation):
    rows = lines(coefficients, col_index[None, :], occupation)
    return sums(planes(rows, col_index))


def solution(mesh):
    return jax.shard_map(
        local,
        mesh=mesh,
        in_specs=(P("band", None, None, "fft"), P(), P("band")),
        out_specs=P("band", "fft", None),
        check_vma=False,
    )
```

```python
import functools
import math

import jax
import jax.numpy as jnp
import numpy as np
from jax import lax
from jax.experimental import pallas as pl
from jax.experimental.pallas import tpu as pltpu
from jax.sharding import PartitionSpec as P

NC = 144
NF = 288
KZ = 72
R = 36
NCOLS = 5184
LC = 648
NP = 18
HALF = 768
FIRST = (0, 5, 9, 14)
COUNT = (5, 4, 5, 4)
LINES_VMEM = 32 * 2**20
GRID_VMEM = 16 * 2**20
DENSITY_VMEM = 32 * 2**20
BF16 = jnp.bfloat16
F32 = jnp.float32
MESH = pl.DeviceIdType.MESH


def hi_lo(table):
    table = np.asarray(table, np.float64)
    hi = table.astype(np.float32).astype(jnp.bfloat16)
    lo = (table - hi.astype(np.float64)).astype(np.float32).astype(jnp.bfloat16)
    return hi, lo


def phases(points):
    k = np.arange(KZ) - R
    ang = 2.0 * np.pi * ((k[:, None] * np.arange(points)[None, :]) % points) / points
    return np.cos(ang), np.sin(ang)


def interpolation():
    d = np.arange(NF)[:, None] - 2 * np.arange(NC)[None, :]
    k = np.arange(1, NC // 2)
    ang = 2.0 * np.pi * ((d[:, :, None] * k) % NF) / NF
    return (1.0 + 2.0 * np.cos(ang).sum(axis=2)) / NC


def line_table():
    cos, sin = phases(NC)
    w = np.zeros((2, KZ, 3, 128))
    for d in range(32):
        n, z = COUNT[d % 4], NP * (d // 4) + FIRST[d % 4]
        c, s = cos[:, z : z + n], sin[:, z : z + n]
        t, lane = d // 12, 10 * (d % 12)
        w[0, :, t, lane : lane + n] = c
        w[1, :, t, lane : lane + n] = -s
        w[0, :, t, lane + 5 : lane + 5 + n] = s
        w[1, :, t, lane + 5 : lane + 5 + n] = c
    return np.concatenate(hi_lo(w.reshape(2 * KZ, 384)), axis=0)


def stacked(table):
    hi, lo = hi_lo(table)
    return np.concatenate([hi, hi, lo], axis=1)


def first_table():
    cos, sin = phases(NC)
    return stacked(np.block([[cos.T, -sin.T], [sin.T, cos.T]]))


def second_tables():
    cos, sin = phases(NC)
    ch, cl = hi_lo(cos)
    sh, sl = hi_lo(sin)
    return ch, cl, sh, sl


def owner_rows():
    m = interpolation()
    rows = np.zeros((8, 5, 8, NC))
    for zc in range(8):
        for y in range(2):
            for c in range(2):
                g = NC * y + 18 * zc + 9 * c
                rows[zc, 2 * y + c] = m[g : g + 8]
                rows[zc, 4, 2 * y + c] = rows[zc, 4, 4 + 2 * y + c] = m[g + 8]
    return stacked(rows.reshape(320, NC))


def split(x):
    hi = x.astype(BF16)
    lo = (x - hi.astype(F32)).astype(BF16)
    return hi, lo


def dot(a, b):
    return jnp.dot(a, b, preferred_element_type=F32)


CHIPS = sorted(
    ((dx, dy) for dx in range(4) for dy in range(4)),
    key=lambda d: (-min(d[0], 4 - d[0]) - min(d[1], 4 - d[1]), d),
)
TARGETS = [(dx, dy, dc) for dx, dy in CHIPS for dc in (1, 0) if (dx, dy, dc) != (0, 0, 0)]


def load_tables(pairs, sems):
    loads = [pltpu.make_async_copy(src, dst, sems.at[i]) for i, (src, dst) in enumerate(pairs)]
    for one in loads:
        one.start()
    return loads


def lines_kernel(
    coef_hbm, cols_hbm, occ_ref, w_hbm, out_ref,
    coef, cols, w, lanes, given, got, load, give_s, got_r,
):
    loads = load_tables(((cols_hbm, cols), (coef_hbm, coef), (w_hbm, w)), load)
    band, me = lax.axis_index("band"), lax.axis_index("fft")
    yh, zc, c = band // 16, (band // 2) % 8, band % 2
    x, y = me // 2, 2 * yh + me % 2
    slot = 4 * me + 2 * yh + c

    def device(xx, yy, cc):
        return {"band": (yy // 2) * 16 + zc * 2 + cc, "fft": 2 * xx + yy % 2}

    targets = [((x + dx) % 4, (y + dy) % 4, (c + dc) % 2) for dx, dy, dc in TARGETS]
    barrier = pltpu.get_barrier_semaphore()
    for target in targets:
        pl.semaphore_signal(barrier, inc=1, device_id=device(*target), device_id_type=MESH)

    loads[0].wait()
    window = cols[:, pl.ds(pl.multiple_of(640 * me, 128), 704)]
    window = jnp.concatenate([window, window[:, 0:64]], axis=1)
    box = pltpu.roll(window, lax.rem(768 - 8 * me, 768), 1)[:, 0:LC].astype(F32)
    k0 = jnp.floor((box + 0.5) * (1.0 / KZ))
    k1 = box - KZ * k0 - R
    k0 = k0 - R
    k = lax.broadcasted_iota(jnp.int32, (KZ, LC), 0).astype(F32) - R
    inside = k * k + (k0 * k0 + k1 * k1) <= float(R * R)
    scale = jnp.sqrt(jnp.full((1, LC), occ_ref[0].astype(F32) * (1.0 / 32.0)))
    scale = jnp.where(inside, scale, 0.0)
    for one in loads[1:]:
        one.wait()
    xt = jnp.concatenate([coef[0, 0] * scale, coef[0, 1] * scale], axis=0).T
    hi, lo = split(xt)
    wh, wl = w[0 : 2 * KZ], w[2 * KZ : 4 * KZ]
    value = dot(hi, wh) + dot(lo, wh) + dot(hi, wl)
    for t in range(3):
        lanes[t] = value[:, 128 * t : 128 * (t + 1)]
    lane = lax.broadcasted_iota(jnp.int32, (56, 128), 1)
    pieces = [(q, 56 if q < 11 else 32) for q in range(12)]

    group = jnp.zeros((56, 128), jnp.int32)
    for q in range(1, 12):
        group = group + (lane >= 10 * q).astype(jnp.int32)
    mine = 2 * yh + c

    def packed(d):
        t, e = d // 12, d % 12
        tile = lanes.at[t]
        result = None
        for q, n in pieces:
            m = lax.rem(q + mine, 12)
            turned = pltpu.roll(tile[56 * q : 56 * q + n, :], lax.rem(1280 + 10 * m - 10 * e, 128), 1)
            if n < 56:
                turned = jnp.concatenate([turned, jnp.zeros((56 - n, 128), F32)], axis=0)
            result = turned if result is None else jnp.where(group == m, turned, result)
        return result

    moves = {}
    for i, target in enumerate(targets):
        xx, yy, cc = target
        given[i] = packed(4 * (2 * xx + yy % 2) + 2 * (yy // 2) + cc)
        if i == 0:
            pl.semaphore_wait(barrier, len(targets))
        move = pltpu.make_async_remote_copy(
            src_ref=given.at[i], dst_ref=got.at[slot],
            send_sem=give_s.at[i], recv_sem=got_r.at[i], device_id=device(*target), device_id_type=MESH,
        )
        move.start()
        moves[TARGETS[i]] = move
    got[slot] = packed(slot)

    def unpack(f):
        base = pl.multiple_of(f * LC, 8)
        for q, n in pieces:
            blocks = [got[4 * f + i, 0:n, :] for i in range(4)]
            here = lane[0:n]
            straight = min(4, 12 - q)
            first = blocks[0]
            for i in range(1, straight):
                first = jnp.where(here >= 10 * (q + i), blocks[i], first)
            result = pltpu.roll(first, 128 - 10 * q, 1) if q else first
            if straight < 4:
                second = blocks[straight]
                for i in range(straight + 1, 4):
                    second = jnp.where(here >= 10 * (q + i - 12), blocks[i], second)
                second = pltpu.roll(second, 120 - 10 * q, 1) if q < 12 else second
                result = jnp.where(here >= 10 * straight, second, result)
            out_ref[pl.ds(base + 56 * q, n), :] = result

    for dx, odd in ((0, 1), (0, 0), (1, 1), (3, 1), (1, 0), (3, 0), (2, 1), (2, 0)):
        for dy in (odd, odd + 2):
            for dc in (0, 1):
                if (dx, dy, dc) in moves:
                    moves[dx, dy, dc].wait_recv()
        unpack(((x + 4 - dx) % 4) * 2 + (y + odd) % 2)
    for move in moves.values():
        move.wait_send()


def lines(coefficients, cols, occ):
    w = line_table()
    hbm = pl.BlockSpec(memory_space=pltpu.HBM)
    dma = pltpu.SemaphoreType.DMA
    n = len(TARGETS)
    return pl.pallas_call(
        lines_kernel,
        out_shape=jax.ShapeDtypeStruct((NCOLS, 128), F32),
        in_specs=[hbm, hbm, pl.BlockSpec(memory_space=pltpu.SMEM), hbm],
        out_specs=pl.BlockSpec(memory_space=pltpu.VMEM),
        scratch_shapes=[
            pltpu.VMEM((1, 2, KZ, LC), F32),
            pltpu.VMEM((1, NCOLS), jnp.int32),
            pltpu.VMEM((4 * KZ, 384), BF16),
            pltpu.VMEM((3, LC, 128), F32),
            pltpu.VMEM((n, 56, 128), F32),
            pltpu.VMEM((32, 56, 128), F32),
            dma((3,)), dma((n,)), dma((n,)),
        ],
        compiler_params=pltpu.CompilerParams(
            collective_id=1, has_side_effects=True, vmem_limit_bytes=LINES_VMEM
        ),
    )(coefficients, cols, occ, jnp.asarray(w))


def grid_kernel(rows_ref, cols_ref, out_ref, grid_ref):
    def scatter(i, carry):
        for u in range(16):
            n = i * 16 + u
            grid_ref[pl.ds(cols_ref[n], 1), :] = rows_ref[pl.ds(n, 1), :]
        return carry

    lax.fori_loop(0, NCOLS // 16, scatter, 0)

    def turn(i, carry):
        for u in range(8):
            k0 = i * 8 + u
            t = grid_ref[pl.ds(pl.multiple_of(k0 * KZ, 8), 128), :].T
            out_ref[pl.ds(k0, 40, stride=KZ), :] = t[0:40]
        return carry

    lax.fori_loop(0, KZ // 8, turn, 0)


def grid(rows, cols):
    vmem = pl.BlockSpec(memory_space=pltpu.VMEM)
    return pl.pallas_call(
        grid_kernel,
        out_shape=jax.ShapeDtypeStruct((40 * KZ, 128), F32),
        in_specs=[vmem, pl.BlockSpec(memory_space=pltpu.SMEM)],
        out_specs=vmem,
        scratch_shapes=[pltpu.VMEM((NCOLS + 56, 128), F32)],
        compiler_params=pltpu.CompilerParams(vmem_limit_bytes=GRID_VMEM),
    )(rows, cols)


def density_kernel(
    g_ref, ch_hbm, cl_hbm, sh_hbm, sl_hbm, t2_hbm, m3_hbm, mh_hbm, ml_hbm, out_ref,
    ch_ref, cl_ref, sh_ref, sl_ref, t2_ref, m3_ref, mh_ref, ml_ref,
    hall_ref, part, held, sent, acc, left, fine, packed, given, got, turned,
    load, ring_s, ring_r, got_s, got_r,
):
    loads = load_tables(
        (
            (ch_hbm, ch_ref), (cl_hbm, cl_ref), (sh_hbm, sh_ref), (sl_hbm, sl_ref),
            (t2_hbm, t2_ref), (m3_hbm, m3_ref), (mh_hbm, mh_ref), (ml_hbm, ml_ref),
        ),
        load,
    )
    band, me = lax.axis_index("band"), lax.axis_index("fft")
    yh, zc, c = band // 16, (band // 2) % 8, band % 2
    x, y = me // 2, 2 * yh + me % 2
    slot = 4 * me + 2 * yh + c

    def device(xx, yy, cc):
        return {"band": (yy // 2) * 16 + zc * 2 + cc, "fft": 2 * xx + yy % 2}

    ring_to = [{"band": yh * 16 + ((zc + d) % 8) * 2 + c, "fft": me} for d in (7, 1)]
    targets = [((x + dx) % 4, (y + dy) % 4, (c + dc) % 2) for dx, dy, dc in TARGETS]
    barrier = pltpu.get_barrier_semaphore()
    for where in [*ring_to, *(device(*target) for target in targets)]:
        pl.semaphore_signal(barrier, inc=1, device_id=where, device_id_type=MESH)

    started = []

    def copy(src, dst, send, recv, where):
        made = pltpu.make_async_remote_copy(
            src_ref=src, dst_ref=dst, send_sem=send, recv_sem=recv, device_id=where, device_id_type=MESH
        )
        made.start()
        started.append(made)
        return made

    for one in loads:
        one.wait()
    ch, cl, sh, sl = ch_ref[...], cl_ref[...], sh_ref[...], sl_ref[...]
    rows = 5 * KZ
    for h in range(4):
        hall_ref[:, HALF * h + 5 * NC : HALF * (h + 1)] = jnp.zeros((NC, HALF - 5 * NC), F32)
        base = 10 * h * KZ
        re_h, re_l = split(g_ref[base : base + rows, 0:KZ])
        im_h, im_l = split(g_ref[base + rows : base + 2 * rows, 0:KZ])
        half_re = (dot(re_h, ch) + dot(re_l, ch) + dot(re_h, cl)) - (
            dot(im_h, sh) + dot(im_l, sh) + dot(im_h, sl)
        )
        half_im = (dot(re_h, sh) + dot(re_l, sh) + dot(re_h, sl)) + (
            dot(im_h, ch) + dot(im_l, ch) + dot(im_h, cl)
        )
        for u in range(5):
            at = HALF * h + NC * u
            hall_ref[0:KZ, at : at + NC] = half_re[KZ * u : KZ * (u + 1)]
            hall_ref[KZ : 2 * KZ, at : at + NC] = half_im[KZ * u : KZ * (u + 1)]

    row = lax.broadcasted_iota(jnp.int32, (8, 128), 0)

    def chunk(t):
        total = 0.0
        for h in range(4):
            field = [hall_ref[:, HALF * h + 128 * i : HALF * h + 128 * (i + 1)] for i in (t, t + 3)]
            hh, hl = split(jnp.concatenate(field, axis=1))
            psi = dot(t2_ref[...], jnp.concatenate([hh, hl, hh], axis=0))
            re, im = psi[0:NC], psi[NC : 2 * NC]
            total = total + (re * re + im * im)
        dh, dl = split(total)
        both = dot(m3_ref[...], jnp.concatenate([dh, dl, dh], axis=0))
        first, second = both[:, 0:128].reshape(8, 5, 8, 128), both[:, 128:256].reshape(8, 5, 8, 128)
        for p in range(4):
            part[:, t, 2 * p] = first[:, p]
            part[:, t, 2 * p + 1] = second[:, p]
        part[:, t, 8] = jnp.where(row[None] < 4, first[:, 4], second[:, 4])

    alone = (pl.ds(0, 4), pl.ds(4, 5))
    ring = {}

    def hop(step, t):
        for way in range(2):
            away = 4 - step
            owner = (zc + (8 - away if way == 0 else away)) % 8
            units = alone[way] if step == 0 else pl.ds(0, 9)
            if step == 0:
                src = part.at[owner, t, units]
            else:
                ring[way, step - 1, t].wait_recv()
                src = sent.at[way, step, t]
                if step == 1:
                    rest = alone[1 - way]
                    sent[way, step, t, rest] = part[owner, t, rest]
                    sent[way, step, t, alone[way]] = part[owner, t, alone[way]] + held[way, 0, t, alone[way]]
                else:
                    sent[way, step, t] = part[owner, t] + held[way, step - 1, t]
            ring[way, step, t] = copy(
                src, held.at[way, step, t, units], ring_s.at[way, step, t], ring_r.at[way, step, t], ring_to[way]
            )

    def final(t):
        for way in range(2):
            ring[way, 3, t].wait_recv()
        acc[t] = part[zc, t] + held[0, 3, t] + held[1, 3, t]

    chunk(0)
    pl.semaphore_wait(barrier, len(targets) + 2)
    hop(0, 0)
    chunk(1)
    hop(0, 1)
    hop(1, 0)
    chunk(2)
    hop(0, 2)
    hop(1, 1)
    hop(2, 0)
    hop(1, 2)
    hop(2, 1)
    hop(3, 0)
    hop(2, 2)
    hop(3, 1)
    hop(3, 2)
    for t in range(3):
        final(t)

    for o in range(4):
        main = jnp.concatenate([acc[t, 2 * o] for t in range(3)] + [acc[t, 2 * o + 1] for t in range(3)], axis=1)
        ninth = jnp.concatenate(
            [acc[t, 8, o : o + 1, :] for t in range(3)] + [acc[t, 8, 4 + o : 5 + o, :] for t in range(3)], axis=1
        )
        for u in range(5):
            n = 5 * o + u
            left[8 * n : 8 * n + 8, :] = main[:, NC * u : NC * (u + 1)]
            left[160 + n : 161 + n, :] = ninth[:, NC * u : NC * (u + 1)]
    lh, ll = split(left[...])
    mh, ml = mh_ref[...], ml_ref[...]
    value = dot(lh, mh) + dot(ll, mh) + dot(lh, ml)
    for t in range(3):
        fine[t, :, 0 : min(128, NF - 128 * t)] = value[:, 128 * t : min(128 * (t + 1), NF)]
    for o in range(4):
        for g in range(9):
            here = pl.ds(40 * o + g, 5, stride=8) if g < 8 else pl.ds(160 + 5 * o, 5)
            line = jnp.concatenate([fine[t, here, :] for t in range(3)], axis=1)
            for j in range(8):
                packed[j, o, 0:5, 36 * g : 36 * g + 36] = line[:, 36 * j : 36 * j + 36]
    for j in range(8):
        for o in range(4):
            for t in range(3):
                given[4 * j + o, 5 * t : 5 * t + 5, :] = packed[j, o, 0:5, 128 * t : 128 * (t + 1)]
    moves = []
    for i, target in enumerate(targets):
        xx, yy, cc = target
        to = 4 * (2 * xx + yy % 2) + 2 * (yy // 2) + cc
        moves.append(copy(given.at[to], got.at[slot], got_s.at[i], got_r.at[i], device(*target)))
    got[slot] = given[slot]
    for one in moves:
        one.wait_recv()
    for j in range(8):
        for o in range(4):
            z = NP * j + FIRST[o]
            for t in range(3):
                turned[z : z + COUNT[o], 128 * t : 128 * (t + 1)] = got[4 * j + o, 5 * t : 5 * t + COUNT[o], :]
    rh, rl = split(turned[...].T)
    for g in range(9):
        a, b = rh[36 * g : 36 * g + 36], rl[36 * g : 36 * g + 36]
        out_ref[g] = dot(a, mh) + dot(b, mh) + dot(a, ml)
    for one in started:
        one.wait_send()


def density(g):
    ch, cl, sh, sl = second_tables()
    mh, ml = hi_lo(interpolation().T)
    tables = (ch, cl, sh, sl, first_table(), owner_rows(), mh, ml)
    vmem = pl.BlockSpec(memory_space=pltpu.VMEM)
    dma = pltpu.SemaphoreType.DMA
    n = len(TARGETS)
    return pl.pallas_call(
        density_kernel,
        out_shape=jax.ShapeDtypeStruct((9, 36, NF), F32),
        in_specs=[vmem] + [pl.BlockSpec(memory_space=pltpu.HBM)] * 8,
        out_specs=vmem,
        scratch_shapes=[
            *(pltpu.VMEM(t.shape, BF16) for t in tables),
            pltpu.VMEM((NC, 4 * HALF), F32),
            pltpu.VMEM((8, 3, 9, 8, 128), F32),
            pltpu.VMEM((2, 4, 3, 9, 8, 128), F32),
            pltpu.VMEM((2, 4, 3, 9, 8, 128), F32),
            pltpu.VMEM((3, 9, 8, 128), F32),
            pltpu.VMEM((184, NC), F32),
            pltpu.VMEM((3, 184, 128), F32),
            pltpu.VMEM((8, 4, 8, 384), F32),
            pltpu.VMEM((32, 16, 128), F32),
            pltpu.VMEM((32, 16, 128), F32),
            pltpu.VMEM((NC, 384), F32),
            dma((8,)),
            dma((2, 4, 3)), dma((2, 4, 3)),
            dma((n,)), dma((n,)),
        ],
        compiler_params=pltpu.CompilerParams(
            collective_id=0, has_side_effects=True, vmem_limit_bytes=DENSITY_VMEM
        ),
    )(g, *(jnp.asarray(t) for t in tables))


def local(coefficients, col_index, occupation):
    rows = lines(coefficients, col_index[None, :], occupation)
    return density(grid(rows, col_index))


def solution(mesh):
    return jax.shard_map(
        local,
        mesh=mesh,
        in_specs=(P("band", None, None, "fft"), P(), P("band")),
        out_specs=P("band", "fft", None),
        check_vma=False,
    )
```

```python
import functools
import math

import jax
import jax.numpy as jnp
import numpy as np
from jax import lax
from jax.experimental import pallas as pl
from jax.experimental.pallas import tpu as pltpu
from jax.sharding import PartitionSpec as P

NC = 144
NF = 288
KZ = 72
R = 36
NCOLS = 5184
LC = 648
NP = 18
HALF = 768
FIRST = (0, 5, 9, 14)
COUNT = (5, 4, 5, 4)
LINES_VMEM = 32 * 2**20
GRID_VMEM = 16 * 2**20
DENSITY_VMEM = 32 * 2**20
BF16 = jnp.bfloat16
F32 = jnp.float32
MESH = pl.DeviceIdType.MESH


def hi_lo(table):
    table = np.asarray(table, np.float64)
    hi = table.astype(np.float32).astype(jnp.bfloat16)
    lo = (table - hi.astype(np.float64)).astype(np.float32).astype(jnp.bfloat16)
    return hi, lo


def phases(points):
    k = np.arange(KZ) - R
    ang = 2.0 * np.pi * ((k[:, None] * np.arange(points)[None, :]) % points) / points
    return np.cos(ang), np.sin(ang)


def interpolation():
    d = np.arange(NF)[:, None] - 2 * np.arange(NC)[None, :]
    k = np.arange(1, NC // 2)
    ang = 2.0 * np.pi * ((d[:, :, None] * k) % NF) / NF
    return (1.0 + 2.0 * np.cos(ang).sum(axis=2)) / NC


def line_table():
    cos, sin = phases(NC)
    w = np.zeros((2, KZ, 3, 128))
    for d in range(32):
        n, z = COUNT[d % 4], NP * (d // 4) + FIRST[d % 4]
        c, s = cos[:, z : z + n], sin[:, z : z + n]
        t, lane = d // 12, 10 * (d % 12)
        w[0, :, t, lane : lane + n] = c
        w[1, :, t, lane : lane + n] = -s
        w[0, :, t, lane + 5 : lane + 5 + n] = s
        w[1, :, t, lane + 5 : lane + 5 + n] = c
    return np.concatenate(hi_lo(w.reshape(2 * KZ, 384)), axis=0)


def stacked(table):
    hi, lo = hi_lo(table)
    return np.concatenate([hi, hi, lo], axis=1)


def first_table():
    cos, sin = phases(NC)
    return stacked(np.block([[cos.T, -sin.T], [sin.T, cos.T]]))


def second_tables():
    cos, sin = phases(NC)
    ch, cl = hi_lo(cos)
    sh, sl = hi_lo(sin)
    return ch, cl, sh, sl


def owner_rows():
    m = interpolation()
    rows = np.zeros((8, 5, 8, NC))
    for zc in range(8):
        for y in range(2):
            for c in range(2):
                g = NC * y + 18 * zc + 9 * c
                rows[zc, 2 * y + c] = m[g : g + 8]
                rows[zc, 4, 2 * y + c] = rows[zc, 4, 4 + 2 * y + c] = m[g + 8]
    return stacked(rows.reshape(320, NC))


def split(x):
    hi = x.astype(BF16)
    lo = (x - hi.astype(F32)).astype(BF16)
    return hi, lo


def dot(a, b):
    return jnp.dot(a, b, preferred_element_type=F32)


CHIPS = sorted(
    ((dx, dy) for dx in range(4) for dy in range(4)),
    key=lambda d: (-min(d[0], 4 - d[0]) - min(d[1], 4 - d[1]), d),
)
TARGETS = [(dx, dy, dc) for dx, dy in CHIPS for dc in (1, 0) if (dx, dy, dc) != (0, 0, 0)]


def lines_kernel(
    coef, cols, occ_ref, w, out_ref,
    lanes, given, got, give_s, got_r,
):
    band, me = lax.axis_index("band"), lax.axis_index("fft")
    yh, zc, c = band // 16, (band // 2) % 8, band % 2
    x, y = me // 2, 2 * yh + me % 2
    slot = 4 * me + 2 * yh + c

    def device(xx, yy, cc):
        return {"band": (yy // 2) * 16 + zc * 2 + cc, "fft": 2 * xx + yy % 2}

    targets = [((x + dx) % 4, (y + dy) % 4, (c + dc) % 2) for dx, dy, dc in TARGETS]
    barrier = pltpu.get_barrier_semaphore()
    for target in targets:
        pl.semaphore_signal(barrier, inc=1, device_id=device(*target), device_id_type=MESH)

    window = cols[pl.ds(pl.multiple_of(640 * me, 128), 704)].reshape(1, 704)
    window = jnp.concatenate([window, window[:, 0:64]], axis=1)
    box = pltpu.roll(window, lax.rem(768 - 8 * me, 768), 1)[:, 0:LC].astype(F32)
    k0 = jnp.floor((box + 0.5) * (1.0 / KZ))
    k1 = box - KZ * k0 - R
    k0 = k0 - R
    k = lax.broadcasted_iota(jnp.int32, (KZ, LC), 0).astype(F32) - R
    inside = k * k + (k0 * k0 + k1 * k1) <= float(R * R)
    scale = jnp.sqrt(jnp.full((1, LC), occ_ref[0].astype(F32) * (1.0 / 32.0)))
    scale = jnp.where(inside, scale, 0.0)
    xt = jnp.concatenate([coef[0, 0] * scale, coef[0, 1] * scale], axis=0).T
    hi, lo = split(xt)
    wh, wl = w[0 : 2 * KZ], w[2 * KZ : 4 * KZ]
    value = dot(hi, wh) + dot(lo, wh) + dot(hi, wl)
    for t in range(3):
        lanes[t] = value[:, 128 * t : 128 * (t + 1)]
    lane = lax.broadcasted_iota(jnp.int32, (56, 128), 1)
    pieces = [(q, 56 if q < 11 else 32) for q in range(12)]

    group = jnp.zeros((56, 128), jnp.int32)
    for q in range(1, 12):
        group = group + (lane >= 10 * q).astype(jnp.int32)
    mine = 2 * yh + c

    def packed(d):
        t, e = d // 12, d % 12
        tile = lanes.at[t]
        result = None
        for q, n in pieces:
            m = lax.rem(q + mine, 12)
            turned = pltpu.roll(tile[56 * q : 56 * q + n, :], lax.rem(1280 + 10 * m - 10 * e, 128), 1)
            if n < 56:
                turned = jnp.concatenate([turned, jnp.zeros((56 - n, 128), F32)], axis=0)
            result = turned if result is None else jnp.where(group == m, turned, result)
        return result

    moves = {}
    for i, target in enumerate(targets):
        xx, yy, cc = target
        given[i] = packed(4 * (2 * xx + yy % 2) + 2 * (yy // 2) + cc)
        if i == 0:
            pl.semaphore_wait(barrier, len(targets))
        move = pltpu.make_async_remote_copy(
            src_ref=given.at[i], dst_ref=got.at[slot],
            send_sem=give_s.at[i], recv_sem=got_r.at[i], device_id=device(*target), device_id_type=MESH,
        )
        move.start()
        moves[TARGETS[i]] = move
    got[slot] = packed(slot)

    def unpack(f):
        base = pl.multiple_of(f * LC, 8)
        for q, n in pieces:
            blocks = [got[4 * f + i, 0:n, :] for i in range(4)]
            here = lane[0:n]
            straight = min(4, 12 - q)
            first = blocks[0]
            for i in range(1, straight):
                first = jnp.where(here >= 10 * (q + i), blocks[i], first)
            result = pltpu.roll(first, 128 - 10 * q, 1) if q else first
            if straight < 4:
                second = blocks[straight]
                for i in range(straight + 1, 4):
                    second = jnp.where(here >= 10 * (q + i - 12), blocks[i], second)
                second = pltpu.roll(second, 120 - 10 * q, 1) if q < 12 else second
                result = jnp.where(here >= 10 * straight, second, result)
            out_ref[pl.ds(base + 56 * q, n), :] = result

    for dx, odd in ((0, 1), (0, 0), (1, 1), (3, 1), (1, 0), (3, 0), (2, 1), (2, 0)):
        for dy in (odd, odd + 2):
            for dc in (0, 1):
                if (dx, dy, dc) in moves:
                    moves[dx, dy, dc].wait_recv()
        unpack(((x + 4 - dx) % 4) * 2 + (y + odd) % 2)
    for move in moves.values():
        move.wait_send()


def lines(coefficients, cols, occ):
    w = line_table()
    vmem = pl.BlockSpec(memory_space=pltpu.VMEM)
    dma = pltpu.SemaphoreType.DMA
    n = len(TARGETS)
    return pl.pallas_call(
        lines_kernel,
        out_shape=jax.ShapeDtypeStruct((NCOLS, 128), F32),
        in_specs=[vmem, vmem, pl.BlockSpec(memory_space=pltpu.SMEM), vmem],
        out_specs=vmem,
        scratch_shapes=[
            pltpu.VMEM((3, LC, 128), F32),
            pltpu.VMEM((n, 56, 128), F32),
            pltpu.VMEM((32, 56, 128), F32),
            dma((n,)), dma((n,)),
        ],
        compiler_params=pltpu.CompilerParams(
            collective_id=1, has_side_effects=True, vmem_limit_bytes=LINES_VMEM
        ),
    )(coefficients, cols, occ, jnp.asarray(w))


def grid_kernel(rows_ref, cols_ref, out_ref, grid_ref):
    def scatter(i, carry):
        for u in range(144):
            n = i * 144 + u
            grid_ref[pl.ds(cols_ref[n], 1), :] = rows_ref[pl.ds(n, 1), :]
        return carry

    lax.fori_loop(0, NCOLS // 144, scatter, 0)

    def turn(i, carry):
        for u in range(8):
            k0 = i * 8 + u
            t = grid_ref[pl.ds(pl.multiple_of(k0 * KZ, 8), 128), :].T
            out_ref[pl.ds(k0, 40, stride=KZ), :] = t[0:40]
        return carry

    lax.fori_loop(0, KZ // 8, turn, 0)


def grid(rows, cols):
    vmem = pl.BlockSpec(memory_space=pltpu.VMEM)
    return pl.pallas_call(
        grid_kernel,
        out_shape=jax.ShapeDtypeStruct((40 * KZ, 128), F32),
        in_specs=[vmem, pl.BlockSpec(memory_space=pltpu.SMEM)],
        out_specs=vmem,
        scratch_shapes=[pltpu.VMEM((NCOLS + 56, 128), F32)],
        compiler_params=pltpu.CompilerParams(vmem_limit_bytes=GRID_VMEM),
    )(rows, cols)


def density_kernel(
    g_ref, ch_ref, cl_ref, sh_ref, sl_ref, t2_ref, m3_ref, mh_ref, ml_ref, out_ref,
    hall_ref, part, held, sent, acc, left, fine, packed, given, got, turned,
    ring_s, ring_r, got_s, got_r,
):
    band, me = lax.axis_index("band"), lax.axis_index("fft")
    yh, zc, c = band // 16, (band // 2) % 8, band % 2
    x, y = me // 2, 2 * yh + me % 2
    slot = 4 * me + 2 * yh + c

    def device(xx, yy, cc):
        return {"band": (yy // 2) * 16 + zc * 2 + cc, "fft": 2 * xx + yy % 2}

    ring_to = [{"band": yh * 16 + ((zc + d) % 8) * 2 + c, "fft": me} for d in (6, 7, 1, 2)]
    targets = [((x + dx) % 4, (y + dy) % 4, (c + dc) % 2) for dx, dy, dc in TARGETS]
    barrier = pltpu.get_barrier_semaphore()
    for where in [*ring_to, *(device(*target) for target in targets)]:
        pl.semaphore_signal(barrier, inc=1, device_id=where, device_id_type=MESH)

    started = []

    def copy(src, dst, send, recv, where):
        made = pltpu.make_async_remote_copy(
            src_ref=src, dst_ref=dst, send_sem=send, recv_sem=recv, device_id=where, device_id_type=MESH
        )
        made.start()
        started.append(made)
        return made

    ch, cl, sh, sl = ch_ref[...], cl_ref[...], sh_ref[...], sl_ref[...]
    rows = 5 * KZ
    for h in range(4):
        hall_ref[:, HALF * h + 5 * NC : HALF * (h + 1)] = jnp.zeros((NC, HALF - 5 * NC), F32)
        base = 10 * h * KZ
        re_h, re_l = split(g_ref[base : base + rows, 0:KZ])
        im_h, im_l = split(g_ref[base + rows : base + 2 * rows, 0:KZ])
        half_re = (dot(re_h, ch) + dot(re_l, ch) + dot(re_h, cl)) - (
            dot(im_h, sh) + dot(im_l, sh) + dot(im_h, sl)
        )
        half_im = (dot(re_h, sh) + dot(re_l, sh) + dot(re_h, sl)) + (
            dot(im_h, ch) + dot(im_l, ch) + dot(im_h, cl)
        )
        for u in range(5):
            at = HALF * h + NC * u
            hall_ref[0:KZ, at : at + NC] = half_re[KZ * u : KZ * (u + 1)]
            hall_ref[KZ : 2 * KZ, at : at + NC] = half_im[KZ * u : KZ * (u + 1)]

    row = lax.broadcasted_iota(jnp.int32, (8, 128), 0)

    def chunk(t):
        total = 0.0
        for h in range(4):
            field = [hall_ref[:, HALF * h + 128 * i : HALF * h + 128 * (i + 1)] for i in (t, t + 3)]
            hh, hl = split(jnp.concatenate(field, axis=1))
            psi = dot(t2_ref[...], jnp.concatenate([hh, hl, hh], axis=0))
            re, im = psi[0:NC], psi[NC : 2 * NC]
            total = total + (re * re + im * im)
        dh, dl = split(total)
        both = dot(m3_ref[...], jnp.concatenate([dh, dl, dh], axis=0))
        first, second = both[:, 0:128].reshape(8, 5, 8, 128), both[:, 128:256].reshape(8, 5, 8, 128)
        for p in range(4):
            part[:, t, 2 * p] = first[:, p]
            part[:, t, 2 * p + 1] = second[:, p]
        part[:, t, 8] = jnp.where(row[None] < 4, first[:, 4], second[:, 4])

    alone = (pl.ds(0, 4), pl.ds(4, 5))
    ring = {}

    def owner(way, away):
        return (zc + (8 - away if way == 0 else away)) % 8

    def send(way, kind, t, src, units, hops):
        to = {"band": yh * 16 + owner(way, hops) * 2 + c, "fft": me}
        ring[way, kind, t] = copy(
            src, held.at[way, kind, t, units], ring_s.at[way, kind, t], ring_r.at[way, kind, t], to
        )

    def early(t):
        for way in range(2):
            send(way, 0, t, part.at[owner(way, 4), t, alone[way]], alone[way], 2)
        for way in range(2):
            send(way, 1, t, part.at[owner(way, 3), t], pl.ds(0, 9), 1)

    def near(t):
        for way in range(2):
            send(way, 2, t, part.at[owner(way, 1), t], pl.ds(0, 9), 1)

    def joined(t):
        for way in range(2):
            ring[way, 0, t].wait_recv()
            ring[way, 1, t].wait_recv()
            mine, rest = alone[way], alone[1 - way]
            sent[way, t, rest] = part[owner(way, 2), t, rest] + held[way, 1, t, rest]
            sent[way, t, mine] = part[owner(way, 2), t, mine] + held[way, 1, t, mine] + held[way, 0, t, mine]
            send(way, 3, t, sent.at[way, t], pl.ds(0, 9), 2)

    def final(t):
        for way in range(2):
            ring[way, 2, t].wait_recv()
            ring[way, 3, t].wait_recv()
        acc[t] = part[zc, t] + held[0, 2, t] + held[1, 2, t] + held[0, 3, t] + held[1, 3, t]

    chunk(0)
    pl.semaphore_wait(barrier, len(targets) + 4)
    early(0)
    chunk(1)
    early(1)
    chunk(2)
    early(2)
    near(0)
    joined(0)
    near(1)
    joined(1)
    near(2)
    joined(2)
    for t in range(3):
        final(t)

    for o in range(4):
        main = jnp.concatenate([acc[t, 2 * o] for t in range(3)] + [acc[t, 2 * o + 1] for t in range(3)], axis=1)
        ninth = jnp.concatenate(
            [acc[t, 8, o : o + 1, :] for t in range(3)] + [acc[t, 8, 4 + o : 5 + o, :] for t in range(3)], axis=1
        )
        for u in range(5):
            n = 5 * o + u
            left[8 * n : 8 * n + 8, :] = main[:, NC * u : NC * (u + 1)]
            left[160 + n : 161 + n, :] = ninth[:, NC * u : NC * (u + 1)]
    lh, ll = split(left[...])
    mh, ml = mh_ref[...], ml_ref[...]
    value = dot(lh, mh) + dot(ll, mh) + dot(lh, ml)
    for t in range(3):
        fine[t, :, 0 : min(128, NF - 128 * t)] = value[:, 128 * t : min(128 * (t + 1), NF)]
    for o in range(4):
        for g in range(9):
            here = pl.ds(40 * o + g, 5, stride=8) if g < 8 else pl.ds(160 + 5 * o, 5)
            line = jnp.concatenate([fine[t, here, :] for t in range(3)], axis=1)
            for j in range(8):
                packed[j, o, 0:5, 36 * g : 36 * g + 36] = line[:, 36 * j : 36 * j + 36]
    for j in range(8):
        for o in range(4):
            for t in range(3):
                given[4 * j + o, 5 * t : 5 * t + 5, :] = packed[j, o, 0:5, 128 * t : 128 * (t + 1)]
    moves = []
    for i, target in enumerate(targets):
        xx, yy, cc = target
        to = 4 * (2 * xx + yy % 2) + 2 * (yy // 2) + cc
        moves.append(copy(given.at[to], got.at[slot], got_s.at[i], got_r.at[i], device(*target)))
    got[slot] = given[slot]
    for one in moves:
        one.wait_recv()
    for j in range(8):
        for o in range(4):
            z = NP * j + FIRST[o]
            for t in range(3):
                turned[z : z + COUNT[o], 128 * t : 128 * (t + 1)] = got[4 * j + o, 5 * t : 5 * t + COUNT[o], :]
    rh, rl = split(turned[...].T)
    for g in range(9):
        a, b = rh[36 * g : 36 * g + 36], rl[36 * g : 36 * g + 36]
        out_ref[g] = dot(a, mh) + dot(b, mh) + dot(a, ml)
    for one in started:
        one.wait_send()


def density(g):
    ch, cl, sh, sl = second_tables()
    mh, ml = hi_lo(interpolation().T)
    tables = (ch, cl, sh, sl, first_table(), owner_rows(), mh, ml)
    vmem = pl.BlockSpec(memory_space=pltpu.VMEM)
    dma = pltpu.SemaphoreType.DMA
    n = len(TARGETS)
    return pl.pallas_call(
        density_kernel,
        out_shape=jax.ShapeDtypeStruct((9, 36, NF), F32),
        in_specs=[vmem] * 9,
        out_specs=vmem,
        scratch_shapes=[
            pltpu.VMEM((NC, 4 * HALF), F32),
            pltpu.VMEM((8, 3, 9, 8, 128), F32),
            pltpu.VMEM((2, 4, 3, 9, 8, 128), F32),
            pltpu.VMEM((2, 3, 9, 8, 128), F32),
            pltpu.VMEM((3, 9, 8, 128), F32),
            pltpu.VMEM((184, NC), F32),
            pltpu.VMEM((3, 184, 128), F32),
            pltpu.VMEM((8, 4, 8, 384), F32),
            pltpu.VMEM((32, 16, 128), F32),
            pltpu.VMEM((32, 16, 128), F32),
            pltpu.VMEM((NC, 384), F32),
            dma((2, 4, 3)), dma((2, 4, 3)),
            dma((n,)), dma((n,)),
        ],
        compiler_params=pltpu.CompilerParams(
            collective_id=0, has_side_effects=True, vmem_limit_bytes=DENSITY_VMEM
        ),
    )(g, *(jnp.asarray(t) for t in tables))


def local(coefficients, col_index, occupation):
    rows = lines(coefficients, col_index, occupation)
    return density(grid(rows, col_index))


def solution(mesh):
    return jax.shard_map(
        local,
        mesh=mesh,
        in_specs=(P("band", None, None, "fft"), P(), P("band")),
        out_specs=P("band", "fft", None),
        check_vma=False,
    )
```

```python
import functools
import math

import jax
import jax.numpy as jnp
import numpy as np
from jax import lax
from jax.experimental import pallas as pl
from jax.experimental.pallas import tpu as pltpu
from jax.sharding import PartitionSpec as P

NC = 144
NF = 288
KZ = 72
R = 36
NCOLS = 5184
LC = 648
NP = 18
HALF = 768
FIRST = (0, 5, 9, 14)
COUNT = (5, 4, 5, 4)
LINES_VMEM = 32 * 2**20
GRID_VMEM = 16 * 2**20
DENSITY_VMEM = 32 * 2**20
BF16 = jnp.bfloat16
F32 = jnp.float32
MESH = pl.DeviceIdType.MESH


def hi_lo(table):
    table = np.asarray(table, np.float64)
    hi = table.astype(np.float32).astype(jnp.bfloat16)
    lo = (table - hi.astype(np.float64)).astype(np.float32).astype(jnp.bfloat16)
    return hi, lo


def phases(points):
    k = np.arange(KZ) - R
    ang = 2.0 * np.pi * ((k[:, None] * np.arange(points)[None, :]) % points) / points
    return np.cos(ang), np.sin(ang)


def interpolation():
    d = np.arange(NF)[:, None] - 2 * np.arange(NC)[None, :]
    k = np.arange(1, NC // 2)
    ang = 2.0 * np.pi * ((d[:, :, None] * k) % NF) / NF
    return (1.0 + 2.0 * np.cos(ang).sum(axis=2)) / NC


def line_table():
    cos, sin = phases(NC)
    w = np.zeros((2, KZ, 3, 128))
    for d in range(32):
        n, z = COUNT[d % 4], NP * (d // 4) + FIRST[d % 4]
        c, s = cos[:, z : z + n], sin[:, z : z + n]
        t, lane = d // 12, 10 * (d % 12)
        w[0, :, t, lane : lane + n] = c
        w[1, :, t, lane : lane + n] = -s
        w[0, :, t, lane + 5 : lane + 5 + n] = s
        w[1, :, t, lane + 5 : lane + 5 + n] = c
    return np.concatenate(hi_lo(w.reshape(2 * KZ, 384)), axis=0)


def stacked(table):
    hi, lo = hi_lo(table)
    return np.concatenate([hi, hi, lo], axis=1)


def first_table():
    cos, sin = phases(NC)
    return stacked(np.block([[cos.T, -sin.T], [sin.T, cos.T]]))


def second_tables():
    cos, sin = phases(NC)
    ch, cl = hi_lo(cos)
    sh, sl = hi_lo(sin)
    return ch, cl, sh, sl


def owner_rows():
    m = interpolation()
    rows = np.zeros((8, 5, 8, NC))
    for zc in range(8):
        for y in range(2):
            for c in range(2):
                g = NC * y + 18 * zc + 9 * c
                rows[zc, 2 * y + c] = m[g : g + 8]
                rows[zc, 4, 2 * y + c] = rows[zc, 4, 4 + 2 * y + c] = m[g + 8]
    return stacked(rows.reshape(320, NC))


def split(x):
    hi = x.astype(BF16)
    lo = (x - hi.astype(F32)).astype(BF16)
    return hi, lo


def dot(a, b):
    return jnp.dot(a, b, preferred_element_type=F32)


GROUPS = ((0, 0), (1, 0), (3, 0), (0, 1), (1, 1), (3, 1), (2, 0), (2, 1))
TARGETS = [
    (dx, dy, dc)
    for dx, odd in GROUPS
    for dy in (odd + 2, odd)
    for dc in (1, 0)
    if (dx, dy, dc) != (0, 0, 0)
]


def lines_kernel(
    coef, cols, occ_ref, w, out_ref,
    lanes, given, got, give_s, got_r,
):
    band, me = lax.axis_index("band"), lax.axis_index("fft")
    yh, zc, c = band // 16, (band // 2) % 8, band % 2
    x, y = me // 2, 2 * yh + me % 2
    slot = 4 * me + 2 * yh + c

    def device(xx, yy, cc):
        return {"band": (yy // 2) * 16 + zc * 2 + cc, "fft": 2 * xx + yy % 2}

    targets = [((x + dx) % 4, (y + dy) % 4, (c + dc) % 2) for dx, dy, dc in TARGETS]
    barrier = pltpu.get_barrier_semaphore()
    for target in targets:
        pl.semaphore_signal(barrier, inc=1, device_id=device(*target), device_id_type=MESH)

    window = cols[pl.ds(pl.multiple_of(640 * me, 128), 704)].reshape(1, 704)
    window = jnp.concatenate([window, window[:, 0:64]], axis=1)
    box = pltpu.roll(window, lax.rem(768 - 8 * me, 768), 1)[:, 0:LC].astype(F32)
    k0 = jnp.floor((box + 0.5) * (1.0 / KZ))
    k1 = box - KZ * k0 - R
    k0 = k0 - R
    k = lax.broadcasted_iota(jnp.int32, (KZ, LC), 0).astype(F32) - R
    inside = k * k + (k0 * k0 + k1 * k1) <= float(R * R)
    scale = jnp.sqrt(jnp.full((1, LC), occ_ref[0].astype(F32) * (1.0 / 32.0)))
    scale = jnp.where(inside, scale, 0.0)
    xt = jnp.concatenate([coef[0, 0] * scale, coef[0, 1] * scale], axis=0).T
    hi, lo = split(xt)
    wh, wl = w[0 : 2 * KZ], w[2 * KZ : 4 * KZ]
    value = dot(hi, wh) + dot(lo, wh) + dot(hi, wl)
    for t in range(3):
        lanes[t] = value[:, 128 * t : 128 * (t + 1)]
    lane = lax.broadcasted_iota(jnp.int32, (56, 128), 1)
    pieces = [(q, 56 if q < 11 else 32) for q in range(12)]

    group = jnp.zeros((56, 128), jnp.int32)
    for q in range(1, 12):
        group = group + (lane >= 10 * q).astype(jnp.int32)
    mine = 2 * yh + c

    def packed(d):
        t, e = d // 12, d % 12
        tile = lanes.at[t]
        result = None
        for q, n in pieces:
            m = lax.rem(q + mine, 12)
            turned = pltpu.roll(tile[56 * q : 56 * q + n, :], lax.rem(1280 + 10 * m - 10 * e, 128), 1)
            if n < 56:
                turned = jnp.concatenate([turned, jnp.zeros((56 - n, 128), F32)], axis=0)
            result = turned if result is None else jnp.where(group == m, turned, result)
        return result

    moves = {}
    for i, target in enumerate(targets):
        xx, yy, cc = target
        given[i] = packed(4 * (2 * xx + yy % 2) + 2 * (yy // 2) + cc)
        if i == 0:
            pl.semaphore_wait(barrier, len(targets))
        move = pltpu.make_async_remote_copy(
            src_ref=given.at[i], dst_ref=got.at[slot],
            send_sem=give_s.at[i], recv_sem=got_r.at[i], device_id=device(*target), device_id_type=MESH,
        )
        move.start()
        moves[TARGETS[i]] = move
    got[slot] = packed(slot)

    def unpack(f):
        base = pl.multiple_of(f * LC, 8)
        for q, n in pieces:
            blocks = [got[4 * f + i, 0:n, :] for i in range(4)]
            here = lane[0:n]
            straight = min(4, 12 - q)
            first = blocks[0]
            for i in range(1, straight):
                first = jnp.where(here >= 10 * (q + i), blocks[i], first)
            result = pltpu.roll(first, 128 - 10 * q, 1) if q else first
            if straight < 4:
                second = blocks[straight]
                for i in range(straight + 1, 4):
                    second = jnp.where(here >= 10 * (q + i - 12), blocks[i], second)
                second = pltpu.roll(second, 120 - 10 * q, 1) if q < 12 else second
                result = jnp.where(here >= 10 * straight, second, result)
            out_ref[pl.ds(base + 56 * q, n), :] = result

    for dx, odd in GROUPS:
        for dy in (odd + 2, odd):
            for dc in (1, 0):
                if (dx, dy, dc) in moves:
                    moves[dx, dy, dc].wait_recv()
        unpack(((x + 4 - dx) % 4) * 2 + (y + odd) % 2)
    for move in moves.values():
        move.wait_send()


def lines(coefficients, cols, occ):
    w = line_table()
    vmem = pl.BlockSpec(memory_space=pltpu.VMEM)
    dma = pltpu.SemaphoreType.DMA
    n = len(TARGETS)
    return pl.pallas_call(
        lines_kernel,
        out_shape=jax.ShapeDtypeStruct((NCOLS, 128), F32),
        in_specs=[vmem, vmem, pl.BlockSpec(memory_space=pltpu.SMEM), vmem],
        out_specs=vmem,
        scratch_shapes=[
            pltpu.VMEM((3, LC, 128), F32),
            pltpu.VMEM((n, 56, 128), F32),
            pltpu.VMEM((32, 56, 128), F32),
            dma((n,)), dma((n,)),
        ],
        compiler_params=pltpu.CompilerParams(
            collective_id=1, has_side_effects=True, vmem_limit_bytes=LINES_VMEM
        ),
    )(coefficients, cols, occ, jnp.asarray(w))


def grid_kernel(rows_ref, cols_ref, out_ref, grid_ref):
    for n in range(NCOLS):
        grid_ref[pl.ds(cols_ref[n], 1), :] = rows_ref[pl.ds(n, 1), :]

    def turn(i, carry):
        for u in range(8):
            k0 = i * 8 + u
            t = grid_ref[pl.ds(pl.multiple_of(k0 * KZ, 8), 128), :].T
            out_ref[pl.ds(k0, 40, stride=KZ), :] = t[0:40]
        return carry

    lax.fori_loop(0, KZ // 8, turn, 0)


def grid(rows, cols):
    vmem = pl.BlockSpec(memory_space=pltpu.VMEM)
    return pl.pallas_call(
        grid_kernel,
        out_shape=jax.ShapeDtypeStruct((40 * KZ, 128), F32),
        in_specs=[vmem, pl.BlockSpec(memory_space=pltpu.SMEM)],
        out_specs=vmem,
        scratch_shapes=[pltpu.VMEM((NCOLS + 56, 128), F32)],
        compiler_params=pltpu.CompilerParams(vmem_limit_bytes=GRID_VMEM),
    )(rows, cols)


def density_kernel(
    g_ref, ch_ref, cl_ref, sh_ref, sl_ref, t2_ref, m3_ref, mh_ref, ml_ref, out_ref,
    hall_ref, part, held, sent, acc, left, fine, packed, given, got, turned,
    ring_s, ring_r, got_s, got_r,
):
    band, me = lax.axis_index("band"), lax.axis_index("fft")
    yh, zc, c = band // 16, (band // 2) % 8, band % 2
    x, y = me // 2, 2 * yh + me % 2
    slot = 4 * me + 2 * yh + c

    def device(xx, yy, cc):
        return {"band": (yy // 2) * 16 + zc * 2 + cc, "fft": 2 * xx + yy % 2}

    ring_to = [{"band": yh * 16 + ((zc + d) % 8) * 2 + c, "fft": me} for d in (6, 7, 1, 2)]
    targets = [((x + dx) % 4, (y + dy) % 4, (c + dc) % 2) for dx, dy, dc in TARGETS]
    barrier = pltpu.get_barrier_semaphore()
    for where in [*ring_to, *(device(*target) for target in targets)]:
        pl.semaphore_signal(barrier, inc=1, device_id=where, device_id_type=MESH)

    started = []

    def copy(src, dst, send, recv, where):
        made = pltpu.make_async_remote_copy(
            src_ref=src, dst_ref=dst, send_sem=send, recv_sem=recv, device_id=where, device_id_type=MESH
        )
        made.start()
        started.append(made)
        return made

    ch, cl, sh, sl = ch_ref[...], cl_ref[...], sh_ref[...], sl_ref[...]
    for h in range(4):
        hall_ref[:, HALF * h + 5 * NC : HALF * (h + 1)] = jnp.zeros((NC, HALF - 5 * NC), F32)

    def first_transform(start, count):
        rows = count * KZ
        for h in range(4):
            base = (10 * h + start) * KZ
            re_h, re_l = split(g_ref[base : base + rows, 0:KZ])
            base += 5 * KZ
            im_h, im_l = split(g_ref[base : base + rows, 0:KZ])
            half_re = (dot(re_h, ch) + dot(re_l, ch) + dot(re_h, cl)) - (
                dot(im_h, sh) + dot(im_l, sh) + dot(im_h, sl)
            )
            half_im = (dot(re_h, sh) + dot(re_l, sh) + dot(re_h, sl)) + (
                dot(im_h, ch) + dot(im_l, ch) + dot(im_h, cl)
            )
            for u in range(count):
                at = HALF * h + NC * (start + u)
                hall_ref[0:KZ, at : at + NC] = half_re[KZ * u : KZ * (u + 1)]
                hall_ref[KZ : 2 * KZ, at : at + NC] = half_im[KZ * u : KZ * (u + 1)]

    row = lax.broadcasted_iota(jnp.int32, (8, 128), 0)

    def chunk(t):
        first_transform(2 * t, min(2, 5 - 2 * t))
        total = 0.0
        for h in range(4):
            hh, hl = split(hall_ref[:, HALF * h + 256 * t : HALF * h + 256 * (t + 1)])
            psi = dot(t2_ref[...], jnp.concatenate([hh, hl, hh], axis=0))
            re, im = psi[0:NC], psi[NC : 2 * NC]
            total = total + (re * re + im * im)
        dh, dl = split(total)
        both = dot(m3_ref[...], jnp.concatenate([dh, dl, dh], axis=0))
        first, second = both[:, 0:128].reshape(8, 5, 8, 128), both[:, 128:256].reshape(8, 5, 8, 128)
        for p in range(4):
            part[:, t, 2 * p] = first[:, p]
            part[:, t, 2 * p + 1] = second[:, p]
        part[:, t, 8] = jnp.where(row[None] < 4, first[:, 4], second[:, 4])

    alone = (pl.ds(0, 4), pl.ds(4, 5))
    ring = {}

    def owner(way, away):
        return (zc + (8 - away if way == 0 else away)) % 8

    def send(way, kind, t, src, units, hops):
        to = {"band": yh * 16 + owner(way, hops) * 2 + c, "fft": me}
        ring[way, kind, t] = copy(
            src, held.at[way, kind, t, units], ring_s.at[way, kind, t], ring_r.at[way, kind, t], to
        )

    def early(t):
        for way in range(2):
            send(way, 0, t, part.at[owner(way, 4), t, alone[way]], alone[way], 2)
        for way in range(2):
            send(way, 1, t, part.at[owner(way, 3), t], pl.ds(0, 9), 1)

    def near(t):
        for way in range(2):
            send(way, 2, t, part.at[owner(way, 1), t], pl.ds(0, 9), 1)

    def joined(t):
        for way in range(2):
            ring[way, 0, t].wait_recv()
            ring[way, 1, t].wait_recv()
            mine, rest = alone[way], alone[1 - way]
            sent[way, t, rest] = part[owner(way, 2), t, rest] + held[way, 1, t, rest]
            sent[way, t, mine] = part[owner(way, 2), t, mine] + held[way, 1, t, mine] + held[way, 0, t, mine]
            send(way, 3, t, sent.at[way, t], pl.ds(0, 9), 2)

    def final(t):
        for way in range(2):
            ring[way, 2, t].wait_recv()
            ring[way, 3, t].wait_recv()
        acc[t] = part[zc, t] + held[0, 2, t] + held[1, 2, t] + held[0, 3, t] + held[1, 3, t]

    chunk(0)
    pl.semaphore_wait(barrier, len(targets) + 4)
    early(0)
    chunk(1)
    early(1)
    chunk(2)
    early(2)
    near(0)
    joined(0)
    near(1)
    joined(1)
    near(2)
    joined(2)
    for t in range(3):
        final(t)

    for o in range(4):
        main = jnp.concatenate([acc[t, 2 * o + i] for t in range(3) for i in range(2)], axis=1)
        ninth = jnp.concatenate(
            [acc[t, 8, 4 * i + o : 4 * i + o + 1, :] for t in range(3) for i in range(2)], axis=1
        )
        for u in range(5):
            n = 5 * o + u
            left[8 * n : 8 * n + 8, :] = main[:, NC * u : NC * (u + 1)]
            left[160 + n : 161 + n, :] = ninth[:, NC * u : NC * (u + 1)]
    lh, ll = split(left[...])
    mh, ml = mh_ref[...], ml_ref[...]
    value = dot(lh, mh) + dot(ll, mh) + dot(lh, ml)
    for t in range(3):
        fine[t, :, 0 : min(128, NF - 128 * t)] = value[:, 128 * t : min(128 * (t + 1), NF)]
    for o in range(4):
        for g in range(9):
            here = pl.ds(40 * o + g, 5, stride=8) if g < 8 else pl.ds(160 + 5 * o, 5)
            line = jnp.concatenate([fine[t, here, :] for t in range(3)], axis=1)
            for j in range(8):
                packed[j, o, 0:5, 36 * g : 36 * g + 36] = line[:, 36 * j : 36 * j + 36]
    for j in range(8):
        for o in range(4):
            for t in range(3):
                given[4 * j + o, 5 * t : 5 * t + 5, :] = packed[j, o, 0:5, 128 * t : 128 * (t + 1)]
    moves = []
    for i, target in enumerate(targets):
        xx, yy, cc = target
        to = 4 * (2 * xx + yy % 2) + 2 * (yy // 2) + cc
        moves.append(copy(given.at[to], got.at[slot], got_s.at[i], got_r.at[i], device(*target)))
    got[slot] = given[slot]
    for one in moves:
        one.wait_recv()
    for j in range(8):
        for o in range(4):
            z = NP * j + FIRST[o]
            for t in range(3):
                turned[z : z + COUNT[o], 128 * t : 128 * (t + 1)] = got[4 * j + o, 5 * t : 5 * t + COUNT[o], :]
    rh, rl = split(turned[...].T)
    for g in range(9):
        a, b = rh[36 * g : 36 * g + 36], rl[36 * g : 36 * g + 36]
        out_ref[g] = dot(a, mh) + dot(b, mh) + dot(a, ml)
    for one in started:
        one.wait_send()


def density(g):
    ch, cl, sh, sl = second_tables()
    mh, ml = hi_lo(interpolation().T)
    tables = (ch, cl, sh, sl, first_table(), owner_rows(), mh, ml)
    vmem = pl.BlockSpec(memory_space=pltpu.VMEM)
    dma = pltpu.SemaphoreType.DMA
    n = len(TARGETS)
    return pl.pallas_call(
        density_kernel,
        out_shape=jax.ShapeDtypeStruct((9, 36, NF), F32),
        in_specs=[vmem] * 9,
        out_specs=vmem,
        scratch_shapes=[
            pltpu.VMEM((NC, 4 * HALF), F32),
            pltpu.VMEM((8, 3, 9, 8, 128), F32),
            pltpu.VMEM((2, 4, 3, 9, 8, 128), F32),
            pltpu.VMEM((2, 3, 9, 8, 128), F32),
            pltpu.VMEM((3, 9, 8, 128), F32),
            pltpu.VMEM((184, NC), F32),
            pltpu.VMEM((3, 184, 128), F32),
            pltpu.VMEM((8, 4, 8, 384), F32),
            pltpu.VMEM((32, 16, 128), F32),
            pltpu.VMEM((32, 16, 128), F32),
            pltpu.VMEM((NC, 384), F32),
            dma((2, 4, 3)), dma((2, 4, 3)),
            dma((n,)), dma((n,)),
        ],
        compiler_params=pltpu.CompilerParams(
            collective_id=0, has_side_effects=True, vmem_limit_bytes=DENSITY_VMEM
        ),
    )(g, *(jnp.asarray(t) for t in tables))


def local(coefficients, col_index, occupation):
    rows = lines(coefficients, col_index, occupation)
    return density(grid(rows, col_index))


def solution(mesh):
    return jax.shard_map(
        local,
        mesh=mesh,
        in_specs=(P("band", None, None, "fft"), P(), P("band")),
        out_specs=P("band", "fft", None),
        check_vma=False,
    )
```

```python
import functools
import math

import jax
import jax.numpy as jnp
import numpy as np
from jax import lax
from jax.experimental import pallas as pl
from jax.experimental.pallas import tpu as pltpu
from jax.sharding import PartitionSpec as P

NC = 144
NF = 288
KZ = 72
R = 36
NCOLS = 5184
LC = 648
NP = 18
HALF = 768
FIRST = (0, 5, 9, 14)
COUNT = (5, 4, 5, 4)
LINES_VMEM = 32 * 2**20
GRID_VMEM = 16 * 2**20
DENSITY_VMEM = 32 * 2**20
BF16 = jnp.bfloat16
F32 = jnp.float32
MESH = pl.DeviceIdType.MESH


def hi_lo(table):
    table = np.asarray(table, np.float64)
    hi = table.astype(np.float32).astype(jnp.bfloat16)
    lo = (table - hi.astype(np.float64)).astype(np.float32).astype(jnp.bfloat16)
    return hi, lo


def phases(points):
    k = np.arange(KZ) - R
    ang = 2.0 * np.pi * ((k[:, None] * np.arange(points)[None, :]) % points) / points
    return np.cos(ang), np.sin(ang)


def interpolation():
    d = np.arange(NF)[:, None] - 2 * np.arange(NC)[None, :]
    k = np.arange(1, NC // 2)
    ang = 2.0 * np.pi * ((d[:, :, None] * k) % NF) / NF
    return (1.0 + 2.0 * np.cos(ang).sum(axis=2)) / NC


def stacked(table):
    hi, lo = hi_lo(table)
    return np.concatenate([hi, hi, lo], axis=1)


def first_table():
    cos, sin = phases(NC)
    return stacked(np.block([[cos.T, -sin.T], [sin.T, cos.T]]))


def second_tables():
    cos, sin = phases(NC)
    ch, cl = hi_lo(cos)
    sh, sl = hi_lo(sin)
    return ch, cl, sh, sl


def owner_rows():
    m = interpolation()
    rows = np.zeros((8, 5, 8, NC))
    for zc in range(8):
        for y in range(2):
            for c in range(2):
                g = NC * y + 18 * zc + 9 * c
                rows[zc, 2 * y + c] = m[g : g + 8]
                rows[zc, 4, 2 * y + c] = rows[zc, 4, 4 + 2 * y + c] = m[g + 8]
    return stacked(rows.reshape(320, NC))


def split(x):
    hi = x.astype(BF16)
    lo = (x - hi.astype(F32)).astype(BF16)
    return hi, lo


def dot(a, b):
    return jnp.dot(a, b, preferred_element_type=F32)


GROUPS = ((0, 0), (1, 0), (3, 0), (0, 1), (1, 1), (3, 1), (2, 0), (2, 1))
TARGETS = [
    (dx, dy, dc)
    for dx, odd in GROUPS
    for dy in (odd + 2, odd)
    for dc in (1, 0)
    if (dx, dy, dc) != (0, 0, 0)
]


def line_table():
    at = lax.broadcasted_iota(jnp.int32, (1, 384), 1).astype(F32)
    tile = jnp.floor((at + 0.5) * (1.0 / 128))
    at = at - 128 * tile
    place = jnp.floor((at + 0.5) * 0.1)
    part = at - 10 * place
    imag = part >= 5
    plane = jnp.where(imag, part - 5, part)
    owner = 12 * tile + place
    fft = jnp.floor((owner + 0.5) * 0.25)
    quarter = owner - 4 * fft
    first, count = jnp.zeros_like(at), jnp.zeros_like(at)
    for i in range(4):
        first = jnp.where(quarter == i, float(FIRST[i]), first)
        count = jnp.where(quarter == i, float(COUNT[i]), count)
    used = (plane < count) & (place < 12) & (fft < 8)
    z = NP * fft + first + plane
    k = lax.broadcasted_iota(jnp.int32, (KZ, 384), 0).astype(F32) - R
    turns = k * z
    turns = turns - NC * jnp.floor((turns + 0.5) * (1.0 / NC))
    quad = jnp.floor((turns + 18.0) * (1.0 / 36))
    a = (turns - 36 * quad) * (2.0 * np.pi / NC)
    b = a * a
    sin = a * (1 + b * (-1 / 6 + b * (1 / 120 + b * (-1 / 5040 + b * (1 / 362880)))))
    cos = 1 + b * (-1 / 2 + b * (1 / 24 + b * (-1 / 720 + b * (1 / 40320 - b * (1 / 3628800)))))
    odd = (quad == 1) | (quad == 3)
    c, s = jnp.where(odd, sin, cos), jnp.where(odd, cos, sin)
    c = jnp.where((quad == 1) | (quad == 2), -c, c)
    s = jnp.where((quad == 2) | (quad == 3), -s, s)
    c, s = jnp.where(used, c, 0.0), jnp.where(used, s, 0.0)
    return jnp.concatenate([jnp.where(imag, s, c), jnp.where(imag, c, -s)], axis=0)


def lines_kernel(
    coef, cols, occ_ref, out_ref,
    lanes, given, got, give_s, got_r,
):
    band, me = lax.axis_index("band"), lax.axis_index("fft")
    yh, zc, c = band // 16, (band // 2) % 8, band % 2
    x, y = me // 2, 2 * yh + me % 2
    slot = 4 * me + 2 * yh + c

    def device(xx, yy, cc):
        return {"band": (yy // 2) * 16 + zc * 2 + cc, "fft": 2 * xx + yy % 2}

    targets = [((x + dx) % 4, (y + dy) % 4, (c + dc) % 2) for dx, dy, dc in TARGETS]
    barrier = pltpu.get_barrier_semaphore()
    for target in targets:
        pl.semaphore_signal(barrier, inc=1, device_id=device(*target), device_id_type=MESH)

    window = cols[pl.ds(pl.multiple_of(640 * me, 128), 704)].reshape(1, 704)
    window = jnp.concatenate([window, window[:, 0:64]], axis=1)
    box = pltpu.roll(window, lax.rem(768 - 8 * me, 768), 1)[:, 0:LC].astype(F32)
    k0 = jnp.floor((box + 0.5) * (1.0 / KZ))
    k1 = box - KZ * k0 - R
    k0 = k0 - R
    k = lax.broadcasted_iota(jnp.int32, (KZ, LC), 0).astype(F32) - R
    inside = k * k + (k0 * k0 + k1 * k1) <= float(R * R)
    scale = jnp.sqrt(jnp.full((1, LC), occ_ref[0].astype(F32) * (1.0 / 32.0)))
    scale = jnp.where(inside, scale, 0.0)
    xt = jnp.concatenate([coef[0, 0] * scale, coef[0, 1] * scale], axis=0).T
    hi, lo = split(xt)
    wh, wl = split(line_table())
    value = dot(hi, wh) + dot(lo, wh) + dot(hi, wl)
    for t in range(3):
        lanes[t] = value[:, 128 * t : 128 * (t + 1)]
    lane = lax.broadcasted_iota(jnp.int32, (56, 128), 1)
    pieces = [(q, 56 if q < 11 else 32) for q in range(12)]

    group = jnp.zeros((56, 128), jnp.int32)
    for q in range(1, 12):
        group = group + (lane >= 10 * q).astype(jnp.int32)
    mine = 2 * yh + c

    def packed(d):
        t, e = d // 12, d % 12
        tile = lanes.at[t]
        result = None
        for q, n in pieces:
            m = lax.rem(q + mine, 12)
            turned = pltpu.roll(tile[56 * q : 56 * q + n, :], lax.rem(1280 + 10 * m - 10 * e, 128), 1)
            if n < 56:
                turned = jnp.concatenate([turned, jnp.zeros((56 - n, 128), F32)], axis=0)
            result = turned if result is None else jnp.where(group == m, turned, result)
        return result

    moves = {}
    for i, target in enumerate(targets):
        xx, yy, cc = target
        given[i] = packed(4 * (2 * xx + yy % 2) + 2 * (yy // 2) + cc)
        if i == 0:
            pl.semaphore_wait(barrier, len(targets))
        move = pltpu.make_async_remote_copy(
            src_ref=given.at[i], dst_ref=got.at[slot],
            send_sem=give_s.at[i], recv_sem=got_r.at[i], device_id=device(*target), device_id_type=MESH,
        )
        move.start()
        moves[TARGETS[i]] = move
    got[slot] = packed(slot)

    def unpack(f):
        base = pl.multiple_of(f * LC, 8)
        for q, n in pieces:
            blocks = [got[4 * f + i, 0:n, :] for i in range(4)]
            here = lane[0:n]
            straight = min(4, 12 - q)
            first = blocks[0]
            for i in range(1, straight):
                first = jnp.where(here >= 10 * (q + i), blocks[i], first)
            result = pltpu.roll(first, 128 - 10 * q, 1) if q else first
            if straight < 4:
                second = blocks[straight]
                for i in range(straight + 1, 4):
                    second = jnp.where(here >= 10 * (q + i - 12), blocks[i], second)
                second = pltpu.roll(second, 120 - 10 * q, 1) if q < 12 else second
                result = jnp.where(here >= 10 * straight, second, result)
            out_ref[pl.ds(base + 56 * q, n), :] = result

    for dx, odd in GROUPS:
        for dy in (odd + 2, odd):
            for dc in (1, 0):
                if (dx, dy, dc) in moves:
                    moves[dx, dy, dc].wait_recv()
        unpack(((x + 4 - dx) % 4) * 2 + (y + odd) % 2)
    for move in moves.values():
        move.wait_send()


def lines(coefficients, cols, occ):
    vmem = pl.BlockSpec(memory_space=pltpu.VMEM)
    dma = pltpu.SemaphoreType.DMA
    n = len(TARGETS)
    return pl.pallas_call(
        lines_kernel,
        out_shape=jax.ShapeDtypeStruct((NCOLS, 128), F32),
        in_specs=[vmem, vmem, pl.BlockSpec(memory_space=pltpu.SMEM)],
        out_specs=vmem,
        scratch_shapes=[
            pltpu.VMEM((3, LC, 128), F32),
            pltpu.VMEM((n, 56, 128), F32),
            pltpu.VMEM((32, 56, 128), F32),
            dma((n,)), dma((n,)),
        ],
        compiler_params=pltpu.CompilerParams(
            collective_id=1, has_side_effects=True, vmem_limit_bytes=LINES_VMEM
        ),
    )(coefficients, cols, occ)


def grid_kernel(rows_ref, cols_ref, out_ref, grid_ref):
    for n in range(NCOLS):
        grid_ref[pl.ds(cols_ref[n], 1), :] = rows_ref[pl.ds(n, 1), :]

    def turn(i, carry):
        for u in range(24):
            k0 = i * 24 + u
            t = grid_ref[pl.ds(pl.multiple_of(k0 * KZ, 8), KZ), :].T[0:40]
            out_ref[pl.ds(k0, 40, stride=KZ), :] = jnp.concatenate([t, jnp.zeros((40, 128 - KZ), F32)], axis=1)
        return carry

    lax.fori_loop(0, KZ // 24, turn, 0)


def grid(rows, cols):
    vmem = pl.BlockSpec(memory_space=pltpu.VMEM)
    return pl.pallas_call(
        grid_kernel,
        out_shape=jax.ShapeDtypeStruct((40 * KZ, 128), F32),
        in_specs=[vmem, pl.BlockSpec(memory_space=pltpu.SMEM)],
        out_specs=vmem,
        scratch_shapes=[pltpu.VMEM((NCOLS + 56, 128), F32)],
        compiler_params=pltpu.CompilerParams(vmem_limit_bytes=GRID_VMEM),
    )(rows, cols)


RELAY = (0,)


def density_kernel(
    g_ref, ch_ref, cl_ref, sh_ref, sl_ref, t2_ref, m3_ref, mh_ref, ml_ref, out_ref,
    hall_ref, part, held, sent, acc, left, fine, packed, given, got, turned,
    ring_s, ring_r, got_s, got_r,
):
    band, me = lax.axis_index("band"), lax.axis_index("fft")
    yh, zc, c = band // 16, (band // 2) % 8, band % 2
    x, y = me // 2, 2 * yh + me % 2
    slot = 4 * me + 2 * yh + c

    def device(xx, yy, cc):
        return {"band": (yy // 2) * 16 + zc * 2 + cc, "fft": 2 * xx + yy % 2}

    ring_to = [{"band": yh * 16 + ((zc + d) % 8) * 2 + c, "fft": me} for d in (6, 7, 1, 2)]
    targets = [((x + dx) % 4, (y + dy) % 4, (c + dc) % 2) for dx, dy, dc in TARGETS]
    barrier = pltpu.get_barrier_semaphore()
    for where in [*ring_to, *(device(*target) for target in targets)]:
        pl.semaphore_signal(barrier, inc=1, device_id=where, device_id_type=MESH)

    started = []

    def copy(src, dst, send, recv, where):
        made = pltpu.make_async_remote_copy(
            src_ref=src, dst_ref=dst, send_sem=send, recv_sem=recv, device_id=where, device_id_type=MESH
        )
        made.start()
        started.append(made)
        return made

    ch, cl, sh, sl = ch_ref[...], cl_ref[...], sh_ref[...], sl_ref[...]
    for h in range(4):
        hall_ref[:, HALF * h + 5 * NC : HALF * (h + 1)] = jnp.zeros((NC, HALF - 5 * NC), F32)

    def first_transform(start, count):
        rows = count * KZ
        for h in range(4):
            base = (10 * h + start) * KZ
            re_h, re_l = split(g_ref[base : base + rows, 0:KZ])
            base += 5 * KZ
            im_h, im_l = split(g_ref[base : base + rows, 0:KZ])
            half_re = (dot(re_h, ch) + dot(re_l, ch) + dot(re_h, cl)) - (
                dot(im_h, sh) + dot(im_l, sh) + dot(im_h, sl)
            )
            half_im = (dot(re_h, sh) + dot(re_l, sh) + dot(re_h, sl)) + (
                dot(im_h, ch) + dot(im_l, ch) + dot(im_h, cl)
            )
            for u in range(count):
                at = HALF * h + NC * (start + u)
                hall_ref[0:KZ, at : at + NC] = half_re[KZ * u : KZ * (u + 1)]
                hall_ref[KZ : 2 * KZ, at : at + NC] = half_im[KZ * u : KZ * (u + 1)]

    row = lax.broadcasted_iota(jnp.int32, (8, 128), 0)

    def chunk(t):
        first_transform(2 * t, min(2, 5 - 2 * t))
        total = 0.0
        for h in range(4):
            hh, hl = split(hall_ref[:, HALF * h + 256 * t : HALF * h + 256 * (t + 1)])
            psi = dot(t2_ref[...], jnp.concatenate([hh, hl, hh], axis=0))
            re, im = psi[0:NC], psi[NC : 2 * NC]
            total = total + (re * re + im * im)
        dh, dl = split(total)
        both = dot(m3_ref[...], jnp.concatenate([dh, dl, dh], axis=0))
        first, second = both[:, 0:128].reshape(8, 5, 8, 128), both[:, 128:256].reshape(8, 5, 8, 128)
        for p in range(4):
            part[:, t, 2 * p] = first[:, p]
            part[:, t, 2 * p + 1] = second[:, p]
        part[:, t, 8] = jnp.where(row[None] < 4, first[:, 4], second[:, 4])

    alone = (pl.ds(0, 4), pl.ds(4, 5))
    ring = {}

    def owner(way, away):
        return (zc + (8 - away if way == 0 else away)) % 8

    def send(way, kind, t, src, units, hops):
        to = {"band": yh * 16 + owner(way, hops) * 2 + c, "fft": me}
        ring[way, kind, t] = copy(
            src, held.at[way, kind, t, units], ring_s.at[way, kind, t], ring_r.at[way, kind, t], to
        )

    def early(t):
        for way in range(2):
            send(way, 0, t, part.at[owner(way, 4), t, alone[way]], alone[way], 2)
        for way in range(2):
            send(way, 1, t, part.at[owner(way, 3), t], pl.ds(0, 9), 1)

    def near(t):
        for way in range(2):
            send(way, 2, t, part.at[owner(way, 1), t], pl.ds(0, 9), 1)

    def joined(t):
        for way in range(2):
            ring[way, 0, t].wait_recv()
            ring[way, 1, t].wait_recv()
            mine, rest = alone[way], alone[1 - way]
            sent[way, 3, t, rest] = part[owner(way, 2), t, rest] + held[way, 1, t, rest]
            sent[way, 3, t, mine] = part[owner(way, 2), t, mine] + held[way, 1, t, mine] + held[way, 0, t, mine]
            send(way, 3, t, sent.at[way, 3, t], pl.ds(0, 9), 2)

    def hop(step, t):
        for way in range(2):
            src, units = part.at[owner(way, 4 - step), t], pl.ds(0, 9)
            if step == 0:
                src, units = part.at[owner(way, 4), t, alone[way]], alone[way]
            else:
                ring[way, step - 1, t].wait_recv()
                mine, rest = alone[way], alone[1 - way]
                here = owner(way, 4 - step)
                if step == 1:
                    sent[way, 1, t, rest] = part[here, t, rest]
                    sent[way, 1, t, mine] = part[here, t, mine] + held[way, 0, t, mine]
                else:
                    sent[way, step, t] = part[here, t] + held[way, step - 1, t]
                src = sent.at[way, step, t]
            send(way, step, t, src, units, 1)

    def final(t):
        for way in range(2):
            if t not in RELAY:
                ring[way, 2, t].wait_recv()
            ring[way, 3, t].wait_recv()
        value = part[zc, t] + held[0, 3, t] + held[1, 3, t]
        if t not in RELAY:
            value = value + held[0, 2, t] + held[1, 2, t]
        acc[t] = value

    chunk(0)
    pl.semaphore_wait(barrier, len(targets) + 4)
    hop(0, 0)
    chunk(1)
    early(1)
    hop(1, 0)
    chunk(2)
    early(2)
    hop(2, 0)
    near(1)
    joined(1)
    near(2)
    hop(3, 0)
    joined(2)
    for t in (1, 0, 2):
        final(t)

    for o in range(4):
        main = jnp.concatenate([acc[t, 2 * o + i] for t in range(3) for i in range(2)], axis=1)
        ninth = jnp.concatenate(
            [acc[t, 8, 4 * i + o : 4 * i + o + 1, :] for t in range(3) for i in range(2)], axis=1
        )
        for u in range(5):
            n = 5 * o + u
            left[8 * n : 8 * n + 8, :] = main[:, NC * u : NC * (u + 1)]
            left[160 + n : 161 + n, :] = ninth[:, NC * u : NC * (u + 1)]
    lh, ll = split(left[...])
    mh, ml = mh_ref[...], ml_ref[...]
    value = dot(lh, mh) + dot(ll, mh) + dot(lh, ml)
    for t in range(3):
        fine[t, :, 0 : min(128, NF - 128 * t)] = value[:, 128 * t : min(128 * (t + 1), NF)]
    for o in range(4):
        for g in range(9):
            here = pl.ds(40 * o + g, 5, stride=8) if g < 8 else pl.ds(160 + 5 * o, 5)
            line = jnp.concatenate([fine[t, here, :] for t in range(3)], axis=1)
            for j in range(8):
                packed[j, o, 0:5, 36 * g : 36 * g + 36] = line[:, 36 * j : 36 * j + 36]
    for j in range(8):
        for o in range(4):
            for t in range(3):
                given[4 * j + o, 5 * t : 5 * t + 5, :] = packed[j, o, 0:5, 128 * t : 128 * (t + 1)]
    moves = []
    for i, target in enumerate(targets):
        xx, yy, cc = target
        to = 4 * (2 * xx + yy % 2) + 2 * (yy // 2) + cc
        moves.append(copy(given.at[to], got.at[slot], got_s.at[i], got_r.at[i], device(*target)))
    got[slot] = given[slot]
    for one in moves:
        one.wait_recv()
    for j in range(8):
        for o in range(4):
            z = NP * j + FIRST[o]
            for t in range(3):
                turned[z : z + COUNT[o], 128 * t : 128 * (t + 1)] = got[4 * j + o, 5 * t : 5 * t + COUNT[o], :]
    rh, rl = split(turned[...].T)
    for g in range(9):
        a, b = rh[36 * g : 36 * g + 36], rl[36 * g : 36 * g + 36]
        out_ref[g] = dot(a, mh) + dot(b, mh) + dot(a, ml)
    for one in started:
        one.wait_send()


def density(g):
    ch, cl, sh, sl = second_tables()
    mh, ml = hi_lo(interpolation().T)
    tables = (ch, cl, sh, sl, first_table(), owner_rows(), mh, ml)
    vmem = pl.BlockSpec(memory_space=pltpu.VMEM)
    dma = pltpu.SemaphoreType.DMA
    n = len(TARGETS)
    return pl.pallas_call(
        density_kernel,
        out_shape=jax.ShapeDtypeStruct((9, 36, NF), F32),
        in_specs=[vmem] * 9,
        out_specs=vmem,
        scratch_shapes=[
            pltpu.VMEM((NC, 4 * HALF), F32),
            pltpu.VMEM((8, 3, 9, 8, 128), F32),
            pltpu.VMEM((2, 4, 3, 9, 8, 128), F32),
            pltpu.VMEM((2, 4, 3, 9, 8, 128), F32),
            pltpu.VMEM((3, 9, 8, 128), F32),
            pltpu.VMEM((184, NC), F32),
            pltpu.VMEM((3, 184, 128), F32),
            pltpu.VMEM((8, 4, 8, 384), F32),
            pltpu.VMEM((32, 16, 128), F32),
            pltpu.VMEM((32, 16, 128), F32),
            pltpu.VMEM((NC, 384), F32),
            dma((2, 4, 3)), dma((2, 4, 3)),
            dma((n,)), dma((n,)),
        ],
        compiler_params=pltpu.CompilerParams(
            collective_id=0, has_side_effects=True, vmem_limit_bytes=DENSITY_VMEM
        ),
    )(g, *(jnp.asarray(t) for t in tables))


def local(coefficients, col_index, occupation):
    rows = lines(coefficients, col_index, occupation)
    return density(grid(rows, col_index))


def solution(mesh):
    return jax.shard_map(
        local,
        mesh=mesh,
        in_specs=(P("band", None, None, "fft"), P(), P("band")),
        out_specs=P("band", "fft", None),
        check_vma=False,
    )
```

```python
import functools
import math

import jax
import jax.numpy as jnp
import numpy as np
from jax import lax
from jax.experimental import pallas as pl
from jax.experimental.pallas import tpu as pltpu
from jax.sharding import PartitionSpec as P

NC = 144
NF = 288
KZ = 72
R = 36
NCOLS = 5184
LC = 648
NP = 18
HALF = 768
FIRST = (0, 5, 9, 14)
COUNT = (5, 4, 5, 4)
LINES_VMEM = 32 * 2**20
GRID_VMEM = 16 * 2**20
DENSITY_VMEM = 32 * 2**20
BF16 = jnp.bfloat16
F32 = jnp.float32
MESH = pl.DeviceIdType.MESH


def hi_lo(table):
    table = np.asarray(table, np.float64)
    hi = table.astype(np.float32).astype(jnp.bfloat16)
    lo = (table - hi.astype(np.float64)).astype(np.float32).astype(jnp.bfloat16)
    return hi, lo


def phases(points):
    k = np.arange(KZ) - R
    ang = 2.0 * np.pi * ((k[:, None] * np.arange(points)[None, :]) % points) / points
    return np.cos(ang), np.sin(ang)


def interpolation():
    d = np.arange(NF)[:, None] - 2 * np.arange(NC)[None, :]
    k = np.arange(1, NC // 2)
    ang = 2.0 * np.pi * ((d[:, :, None] * k) % NF) / NF
    return (1.0 + 2.0 * np.cos(ang).sum(axis=2)) / NC


def stacked(table):
    hi, lo = hi_lo(table)
    return np.concatenate([hi, hi, lo], axis=1)


def first_table():
    cos, sin = phases(NC)
    return stacked(np.block([[cos.T, -sin.T], [sin.T, cos.T]]))


def second_tables():
    cos, sin = phases(NC)
    ch, cl = hi_lo(cos)
    sh, sl = hi_lo(sin)
    return ch, cl, sh, sl


def owner_rows():
    m = interpolation()
    rows = np.zeros((8, 5, 8, NC))
    for zc in range(8):
        for y in range(2):
            for c in range(2):
                g = NC * y + 18 * zc + 9 * c
                rows[zc, 2 * y + c] = m[g : g + 8]
                rows[zc, 4, 2 * y + c] = rows[zc, 4, 4 + 2 * y + c] = m[g + 8]
    return stacked(rows.reshape(320, NC))


def split(x):
    hi = x.astype(BF16)
    lo = (x - hi.astype(F32)).astype(BF16)
    return hi, lo


def dot(a, b):
    return jnp.dot(a, b, preferred_element_type=F32)


GROUPS = ((0, 0), (1, 0), (3, 0), (0, 1), (1, 1), (3, 1), (2, 0), (2, 1))
TARGETS = [
    (dx, dy, dc)
    for dx, odd in GROUPS
    for dy in (odd + 2, odd)
    for dc in (1, 0)
    if (dx, dy, dc) != (0, 0, 0)
]


def line_table():
    at = lax.broadcasted_iota(jnp.int32, (1, 384), 1).astype(F32)
    tile = jnp.floor((at + 0.5) * (1.0 / 128))
    at = at - 128 * tile
    place = jnp.floor((at + 0.5) * 0.1)
    part = at - 10 * place
    imag = part >= 5
    plane = jnp.where(imag, part - 5, part)
    owner = 12 * tile + place
    fft = jnp.floor((owner + 0.5) * 0.25)
    quarter = owner - 4 * fft
    first, count = jnp.zeros_like(at), jnp.zeros_like(at)
    for i in range(4):
        first = jnp.where(quarter == i, float(FIRST[i]), first)
        count = jnp.where(quarter == i, float(COUNT[i]), count)
    used = (plane < count) & (place < 12) & (fft < 8)
    z = NP * fft + first + plane
    k = lax.broadcasted_iota(jnp.int32, (KZ, 384), 0).astype(F32) - R
    turns = k * z
    turns = turns - NC * jnp.floor((turns + 0.5) * (1.0 / NC))
    quad = jnp.floor((turns + 18.0) * (1.0 / 36))
    a = (turns - 36 * quad) * (2.0 * np.pi / NC)
    b = a * a
    sin = a * (1 + b * (-1 / 6 + b * (1 / 120 + b * (-1 / 5040 + b * (1 / 362880)))))
    cos = 1 + b * (-1 / 2 + b * (1 / 24 + b * (-1 / 720 + b * (1 / 40320 - b * (1 / 3628800)))))
    odd = (quad == 1) | (quad == 3)
    c, s = jnp.where(odd, sin, cos), jnp.where(odd, cos, sin)
    c = jnp.where((quad == 1) | (quad == 2), -c, c)
    s = jnp.where((quad == 2) | (quad == 3), -s, s)
    c, s = jnp.where(used, c, 0.0), jnp.where(used, s, 0.0)
    return jnp.concatenate([jnp.where(imag, s, c), jnp.where(imag, c, -s)], axis=0)


def lines_kernel(
    coef, cols, occ_ref, out_ref,
    lanes, given, got, give_s, got_r,
):
    band, me = lax.axis_index("band"), lax.axis_index("fft")
    yh, zc, c = band // 16, (band // 2) % 8, band % 2
    x, y = me // 2, 2 * yh + me % 2
    slot = 4 * me + 2 * yh + c

    def device(xx, yy, cc):
        return {"band": (yy // 2) * 16 + zc * 2 + cc, "fft": 2 * xx + yy % 2}

    targets = [((x + dx) % 4, (y + dy) % 4, (c + dc) % 2) for dx, dy, dc in TARGETS]
    barrier = pltpu.get_barrier_semaphore()
    for target in targets:
        pl.semaphore_signal(barrier, inc=1, device_id=device(*target), device_id_type=MESH)

    window = cols[pl.ds(pl.multiple_of(640 * me, 128), 704)].reshape(1, 704)
    window = jnp.concatenate([window, window[:, 0:64]], axis=1)
    box = pltpu.roll(window, lax.rem(768 - 8 * me, 768), 1)[:, 0:LC].astype(F32)
    k0 = jnp.floor((box + 0.5) * (1.0 / KZ))
    k1 = box - KZ * k0 - R
    k0 = k0 - R
    k = lax.broadcasted_iota(jnp.int32, (KZ, LC), 0).astype(F32) - R
    inside = k * k + (k0 * k0 + k1 * k1) <= float(R * R)
    scale = jnp.sqrt(jnp.full((1, LC), occ_ref[0].astype(F32) * (1.0 / 32.0)))
    scale = jnp.where(inside, scale, 0.0)
    xt = jnp.concatenate([coef[0, 0] * scale, coef[0, 1] * scale], axis=0).T
    hi, lo = split(xt)
    wh, wl = split(line_table())
    value = dot(hi, wh) + dot(lo, wh) + dot(hi, wl)
    for t in range(3):
        lanes[t] = value[:, 128 * t : 128 * (t + 1)]
    lane = lax.broadcasted_iota(jnp.int32, (56, 128), 1)
    pieces = [(q, 56 if q < 11 else 32) for q in range(12)]

    group = jnp.zeros((56, 128), jnp.int32)
    for q in range(1, 12):
        group = group + (lane >= 10 * q).astype(jnp.int32)
    mine = 2 * yh + c

    def packed(d):
        t, e = d // 12, d % 12
        tile = lanes.at[t]
        result = None
        for q, n in pieces:
            m = lax.rem(q + mine, 12)
            turned = pltpu.roll(tile[56 * q : 56 * q + n, :], lax.rem(1280 + 10 * m - 10 * e, 128), 1)
            if n < 56:
                turned = jnp.concatenate([turned, jnp.zeros((56 - n, 128), F32)], axis=0)
            result = turned if result is None else jnp.where(group == m, turned, result)
        return result

    moves = {}
    for i, target in enumerate(targets):
        xx, yy, cc = target
        given[i] = packed(4 * (2 * xx + yy % 2) + 2 * (yy // 2) + cc)
        if i == 0:
            pl.semaphore_wait(barrier, len(targets))
        move = pltpu.make_async_remote_copy(
            src_ref=given.at[i], dst_ref=got.at[slot],
            send_sem=give_s.at[i], recv_sem=got_r.at[i], device_id=device(*target), device_id_type=MESH,
        )
        move.start()
        moves[TARGETS[i]] = move
    got[slot] = packed(slot)

    def unpack(f):
        base = pl.multiple_of(f * LC, 8)
        for q, n in pieces:
            blocks = [got[4 * f + i, 0:n, :] for i in range(4)]
            here = lane[0:n]
            straight = min(4, 12 - q)
            first = blocks[0]
            for i in range(1, straight):
                first = jnp.where(here >= 10 * (q + i), blocks[i], first)
            result = pltpu.roll(first, 128 - 10 * q, 1) if q else first
            if straight < 4:
                second = blocks[straight]
                for i in range(straight + 1, 4):
                    second = jnp.where(here >= 10 * (q + i - 12), blocks[i], second)
                second = pltpu.roll(second, 120 - 10 * q, 1) if q < 12 else second
                result = jnp.where(here >= 10 * straight, second, result)
            out_ref[pl.ds(base + 56 * q, n), :] = result

    for dx, odd in GROUPS:
        for dy in (odd + 2, odd):
            for dc in (1, 0):
                if (dx, dy, dc) in moves:
                    moves[dx, dy, dc].wait_recv()
        unpack(((x + 4 - dx) % 4) * 2 + (y + odd) % 2)
    for move in moves.values():
        move.wait_send()


def lines(coefficients, cols, occ):
    vmem = pl.BlockSpec(memory_space=pltpu.VMEM)
    dma = pltpu.SemaphoreType.DMA
    n = len(TARGETS)
    return pl.pallas_call(
        lines_kernel,
        out_shape=jax.ShapeDtypeStruct((NCOLS, 128), F32),
        in_specs=[vmem, vmem, pl.BlockSpec(memory_space=pltpu.SMEM)],
        out_specs=vmem,
        scratch_shapes=[
            pltpu.VMEM((3, LC, 128), F32),
            pltpu.VMEM((n, 56, 128), F32),
            pltpu.VMEM((32, 56, 128), F32),
            dma((n,)), dma((n,)),
        ],
        compiler_params=pltpu.CompilerParams(
            collective_id=1, has_side_effects=True, vmem_limit_bytes=LINES_VMEM
        ),
    )(coefficients, cols, occ)


def grid_kernel(rows_ref, cols_ref, out_ref, grid_ref):
    for n in range(NCOLS):
        grid_ref[pl.ds(cols_ref[n], 1), :] = rows_ref[pl.ds(n, 1), :]

    def turn(i, carry):
        for u in range(72):
            k0 = i * 72 + u
            t = grid_ref[pl.ds(pl.multiple_of(k0 * KZ, 8), KZ), :].T[0:40]
            out_ref[pl.ds(k0, 40, stride=KZ), :] = jnp.concatenate([t, jnp.zeros((40, 128 - KZ), F32)], axis=1)
        return carry

    lax.fori_loop(0, KZ // 72, turn, 0)


def grid(rows, cols):
    vmem = pl.BlockSpec(memory_space=pltpu.VMEM)
    return pl.pallas_call(
        grid_kernel,
        out_shape=jax.ShapeDtypeStruct((40 * KZ, 128), F32),
        in_specs=[vmem, pl.BlockSpec(memory_space=pltpu.SMEM)],
        out_specs=vmem,
        scratch_shapes=[pltpu.VMEM((NCOLS + 56, 128), F32)],
        compiler_params=pltpu.CompilerParams(vmem_limit_bytes=GRID_VMEM),
    )(rows, cols)


RELAY = (0,)


def density_kernel(
    g_ref, ch_ref, cl_ref, sh_ref, sl_ref, t2_ref, m3_ref, mh_ref, ml_ref, out_ref,
    hall_ref, part, held, sent, acc, left, fine, packed, given, got, turned,
    ring_s, ring_r, got_s, got_r,
):
    band, me = lax.axis_index("band"), lax.axis_index("fft")
    yh, zc, c = band // 16, (band // 2) % 8, band % 2
    x, y = me // 2, 2 * yh + me % 2
    slot = 4 * me + 2 * yh + c

    def device(xx, yy, cc):
        return {"band": (yy // 2) * 16 + zc * 2 + cc, "fft": 2 * xx + yy % 2}

    ring_to = [{"band": yh * 16 + ((zc + d) % 8) * 2 + c, "fft": me} for d in (6, 7, 1, 2)]
    targets = [((x + dx) % 4, (y + dy) % 4, (c + dc) % 2) for dx, dy, dc in TARGETS]
    barrier = pltpu.get_barrier_semaphore()
    for where in [*ring_to, *(device(*target) for target in targets)]:
        pl.semaphore_signal(barrier, inc=1, device_id=where, device_id_type=MESH)

    started = []

    def copy(src, dst, send, recv, where):
        made = pltpu.make_async_remote_copy(
            src_ref=src, dst_ref=dst, send_sem=send, recv_sem=recv, device_id=where, device_id_type=MESH
        )
        made.start()
        started.append(made)
        return made

    ch, cl, sh, sl = ch_ref[...], cl_ref[...], sh_ref[...], sl_ref[...]
    for h in range(4):
        hall_ref[:, HALF * h + 5 * NC : HALF * (h + 1)] = jnp.zeros((NC, HALF - 5 * NC), F32)

    def first_transform(start, count):
        rows = count * KZ
        for h in range(4):
            base = (10 * h + start) * KZ
            re_h, re_l = split(g_ref[base : base + rows, 0:KZ])
            base += 5 * KZ
            im_h, im_l = split(g_ref[base : base + rows, 0:KZ])
            half_re = (dot(re_h, ch) + dot(re_l, ch) + dot(re_h, cl)) - (
                dot(im_h, sh) + dot(im_l, sh) + dot(im_h, sl)
            )
            half_im = (dot(re_h, sh) + dot(re_l, sh) + dot(re_h, sl)) + (
                dot(im_h, ch) + dot(im_l, ch) + dot(im_h, cl)
            )
            for u in range(count):
                at = HALF * h + NC * (start + u)
                hall_ref[0:KZ, at : at + NC] = half_re[KZ * u : KZ * (u + 1)]
                hall_ref[KZ : 2 * KZ, at : at + NC] = half_im[KZ * u : KZ * (u + 1)]

    row = lax.broadcasted_iota(jnp.int32, (8, 128), 0)

    def chunk(t):
        first_transform(2 * t, min(2, 5 - 2 * t))
        total = 0.0
        for h in range(4):
            hh, hl = split(hall_ref[:, HALF * h + 256 * t : HALF * h + 256 * (t + 1)])
            psi = dot(t2_ref[...], jnp.concatenate([hh, hl, hh], axis=0))
            re, im = psi[0:NC], psi[NC : 2 * NC]
            total = total + (re * re + im * im)
        dh, dl = split(total)
        both = dot(m3_ref[...], jnp.concatenate([dh, dl, dh], axis=0))
        first, second = both[:, 0:128].reshape(8, 5, 8, 128), both[:, 128:256].reshape(8, 5, 8, 128)
        for p in range(4):
            part[:, t, 2 * p] = first[:, p]
            part[:, t, 2 * p + 1] = second[:, p]
        part[:, t, 8] = jnp.where(row[None] < 4, first[:, 4], second[:, 4])

    alone = (pl.ds(0, 4), pl.ds(4, 5))
    ring = {}

    def owner(way, away):
        return (zc + (8 - away if way == 0 else away)) % 8

    def send(way, kind, t, src, units, hops):
        to = {"band": yh * 16 + owner(way, hops) * 2 + c, "fft": me}
        ring[way, kind, t] = copy(
            src, held.at[way, kind, t, units], ring_s.at[way, kind, t], ring_r.at[way, kind, t], to
        )

    def early(t):
        for way in range(2):
            send(way, 0, t, part.at[owner(way, 4), t, alone[way]], alone[way], 2)
        for way in range(2):
            send(way, 1, t, part.at[owner(way, 3), t], pl.ds(0, 9), 1)

    def near(t):
        for way in range(2):
            send(way, 2, t, part.at[owner(way, 1), t], pl.ds(0, 9), 1)

    def joined(t):
        for way in range(2):
            ring[way, 0, t].wait_recv()
            ring[way, 1, t].wait_recv()
            mine, rest = alone[way], alone[1 - way]
            sent[way, 3, t, rest] = part[owner(way, 2), t, rest] + held[way, 1, t, rest]
            sent[way, 3, t, mine] = part[owner(way, 2), t, mine] + held[way, 1, t, mine] + held[way, 0, t, mine]
            send(way, 3, t, sent.at[way, 3, t], pl.ds(0, 9), 2)

    def hop(step, t):
        for way in range(2):
            src, units = part.at[owner(way, 4 - step), t], pl.ds(0, 9)
            if step == 0:
                src, units = part.at[owner(way, 4), t, alone[way]], alone[way]
            else:
                ring[way, step - 1, t].wait_recv()
                mine, rest = alone[way], alone[1 - way]
                here = owner(way, 4 - step)
                if step == 1:
                    sent[way, 1, t, rest] = part[here, t, rest]
                    sent[way, 1, t, mine] = part[here, t, mine] + held[way, 0, t, mine]
                else:
                    sent[way, step, t] = part[here, t] + held[way, step - 1, t]
                src = sent.at[way, step, t]
            send(way, step, t, src, units, 1)

    def final(t):
        for way in range(2):
            if t not in RELAY:
                ring[way, 2, t].wait_recv()
            ring[way, 3, t].wait_recv()
        value = part[zc, t] + held[0, 3, t] + held[1, 3, t]
        if t not in RELAY:
            value = value + held[0, 2, t] + held[1, 2, t]
        acc[t] = value

    chunk(0)
    pl.semaphore_wait(barrier, len(targets) + 4)
    hop(0, 0)
    chunk(1)
    early(1)
    hop(1, 0)
    chunk(2)
    early(2)
    hop(2, 0)
    near(1)
    joined(1)
    near(2)
    hop(3, 0)
    joined(2)
    for t in (1, 0, 2):
        final(t)

    for o in range(4):
        main = jnp.concatenate([acc[t, 2 * o + i] for t in range(3) for i in range(2)], axis=1)
        ninth = jnp.concatenate(
            [acc[t, 8, 4 * i + o : 4 * i + o + 1, :] for t in range(3) for i in range(2)], axis=1
        )
        for u in range(5):
            n = 5 * o + u
            left[8 * n : 8 * n + 8, :] = main[:, NC * u : NC * (u + 1)]
            left[160 + n : 161 + n, :] = ninth[:, NC * u : NC * (u + 1)]
    lh, ll = split(left[...])
    mh, ml = mh_ref[...], ml_ref[...]
    value = dot(lh, mh) + dot(ll, mh) + dot(lh, ml)
    for t in range(3):
        fine[t, :, 0 : min(128, NF - 128 * t)] = value[:, 128 * t : min(128 * (t + 1), NF)]
    for o in range(4):
        for g in range(9):
            here = pl.ds(40 * o + g, 5, stride=8) if g < 8 else pl.ds(160 + 5 * o, 5)
            line = jnp.concatenate([fine[t, here, :] for t in range(3)], axis=1)
            for j in range(8):
                packed[j, o, 0:5, 36 * g : 36 * g + 36] = line[:, 36 * j : 36 * j + 36]
    for j in range(8):
        for o in range(4):
            for t in range(3):
                given[4 * j + o, 5 * t : 5 * t + 5, :] = packed[j, o, 0:5, 128 * t : 128 * (t + 1)]
    moves = []
    farthest = sorted(range(len(targets)), key=lambda i: -sum(min(v, 4 - v) for v in TARGETS[i][:2]))
    for i in farthest:
        xx, yy, cc = targets[i]
        target = targets[i]
        to = 4 * (2 * xx + yy % 2) + 2 * (yy // 2) + cc
        moves.append(copy(given.at[to], got.at[slot], got_s.at[i], got_r.at[i], device(*target)))
    got[slot] = given[slot]
    for one in moves:
        one.wait_recv()
    for j in range(8):
        for o in range(4):
            z = NP * j + FIRST[o]
            for t in range(3):
                turned[z : z + COUNT[o], 128 * t : 128 * (t + 1)] = got[4 * j + o, 5 * t : 5 * t + COUNT[o], :]
    rh, rl = split(turned[...].T)
    value = dot(rh, mh) + dot(rl, mh) + dot(rh, ml)
    for g in range(9):
        out_ref[g] = value[36 * g : 36 * g + 36]
    for one in started:
        one.wait_send()


def density(g):
    ch, cl, sh, sl = second_tables()
    mh, ml = hi_lo(interpolation().T)
    tables = (ch, cl, sh, sl, first_table(), owner_rows(), mh, ml)
    vmem = pl.BlockSpec(memory_space=pltpu.VMEM)
    dma = pltpu.SemaphoreType.DMA
    n = len(TARGETS)
    return pl.pallas_call(
        density_kernel,
        out_shape=jax.ShapeDtypeStruct((9, 36, NF), F32),
        in_specs=[vmem] * 9,
        out_specs=vmem,
        scratch_shapes=[
            pltpu.VMEM((NC, 4 * HALF), F32),
            pltpu.VMEM((8, 3, 9, 8, 128), F32),
            pltpu.VMEM((2, 4, 3, 9, 8, 128), F32),
            pltpu.VMEM((2, 4, 3, 9, 8, 128), F32),
            pltpu.VMEM((3, 9, 8, 128), F32),
            pltpu.VMEM((184, NC), F32),
            pltpu.VMEM((3, 184, 128), F32),
            pltpu.VMEM((8, 4, 8, 384), F32),
            pltpu.VMEM((32, 16, 128), F32),
            pltpu.VMEM((32, 16, 128), F32),
            pltpu.VMEM((NC, 384), F32),
            dma((2, 4, 3)), dma((2, 4, 3)),
            dma((n,)), dma((n,)),
        ],
        compiler_params=pltpu.CompilerParams(
            collective_id=0, has_side_effects=True, vmem_limit_bytes=DENSITY_VMEM
        ),
    )(g, *(jnp.asarray(t) for t in tables))


def local(coefficients, col_index, occupation):
    rows = lines(coefficients, col_index, occupation)
    return density(grid(rows, col_index))


def solution(mesh):
    return jax.shard_map(
        local,
        mesh=mesh,
        in_specs=(P("band", None, None, "fft"), P(), P("band")),
        out_specs=P("band", "fft", None),
        check_vma=False,
    )
```

```python
import functools
import math

import jax
import jax.numpy as jnp
import numpy as np
from jax import lax
from jax.experimental import pallas as pl
from jax.experimental.pallas import tpu as pltpu
from jax.sharding import PartitionSpec as P

NC = 144
NF = 288
KZ = 72
R = 36
NCOLS = 5184
LC = 648
NP = 18
HALF = 768
FIRST = (0, 5, 9, 14)
COUNT = (5, 4, 5, 4)
LINES_VMEM = 32 * 2**20
GRID_VMEM = 16 * 2**20
DENSITY_VMEM = 32 * 2**20
BF16 = jnp.bfloat16
F32 = jnp.float32
MESH = pl.DeviceIdType.MESH


def hi_lo(table):
    table = np.asarray(table, np.float64)
    hi = table.astype(np.float32).astype(jnp.bfloat16)
    lo = (table - hi.astype(np.float64)).astype(np.float32).astype(jnp.bfloat16)
    return hi, lo


def phases(points):
    k = np.arange(KZ) - R
    ang = 2.0 * np.pi * ((k[:, None] * np.arange(points)[None, :]) % points) / points
    return np.cos(ang), np.sin(ang)


def interpolation():
    d = np.arange(NF)[:, None] - 2 * np.arange(NC)[None, :]
    k = np.arange(1, NC // 2)
    ang = 2.0 * np.pi * ((d[:, :, None] * k) % NF) / NF
    return (1.0 + 2.0 * np.cos(ang).sum(axis=2)) / NC


def stacked(table):
    hi, lo = hi_lo(table)
    return np.concatenate([hi, hi, lo], axis=1)


def first_table():
    cos, sin = phases(NC)
    return stacked(np.block([[cos.T, -sin.T], [sin.T, cos.T]]))


def second_tables():
    cos, sin = phases(NC)
    ch, cl = hi_lo(cos)
    sh, sl = hi_lo(sin)
    return ch, cl, sh, sl


def owner_rows():
    m = interpolation()
    rows = np.zeros((8, 5, 8, NC))
    for zc in range(8):
        for y in range(2):
            for c in range(2):
                g = NC * y + 18 * zc + 9 * c
                rows[zc, 2 * y + c] = m[g : g + 8]
                rows[zc, 4, 2 * y + c] = rows[zc, 4, 4 + 2 * y + c] = m[g + 8]
    return stacked(rows.reshape(320, NC))


def split(x):
    hi = x.astype(BF16)
    lo = (x - hi.astype(F32)).astype(BF16)
    return hi, lo


def dot(a, b):
    return jnp.dot(a, b, preferred_element_type=F32)


GROUPS = ((0, 0), (1, 0), (3, 0), (0, 1), (1, 1), (3, 1), (2, 0), (2, 1))
TARGETS = [
    (dx, dy, dc)
    for dx, odd in GROUPS
    for dc in (1, 0)
    for dy in (odd + 2, odd)
    if (dx, dy, dc) != (0, 0, 0)
]


def line_table():
    at = lax.broadcasted_iota(jnp.int32, (1, 384), 1).astype(F32)
    tile = jnp.floor((at + 0.5) * (1.0 / 128))
    at = at - 128 * tile
    place = jnp.floor((at + 0.5) * 0.1)
    part = at - 10 * place
    imag = part >= 5
    plane = jnp.where(imag, part - 5, part)
    owner = 12 * tile + place
    fft = jnp.floor((owner + 0.5) * 0.25)
    quarter = owner - 4 * fft
    first, count = jnp.zeros_like(at), jnp.zeros_like(at)
    for i in range(4):
        first = jnp.where(quarter == i, float(FIRST[i]), first)
        count = jnp.where(quarter == i, float(COUNT[i]), count)
    used = (plane < count) & (place < 12) & (fft < 8)
    z = NP * fft + first + plane
    k = lax.broadcasted_iota(jnp.int32, (KZ, 384), 0).astype(F32) - R
    turns = k * z
    turns = turns - NC * jnp.floor((turns + 0.5) * (1.0 / NC))
    quad = jnp.floor((turns + 18.0) * (1.0 / 36))
    a = (turns - 36 * quad) * (2.0 * np.pi / NC)
    b = a * a
    sin = a * (1 + b * (-1 / 6 + b * (1 / 120 + b * (-1 / 5040 + b * (1 / 362880)))))
    cos = 1 + b * (-1 / 2 + b * (1 / 24 + b * (-1 / 720 + b * (1 / 40320 - b * (1 / 3628800)))))
    odd = (quad == 1) | (quad == 3)
    c, s = jnp.where(odd, sin, cos), jnp.where(odd, cos, sin)
    c = jnp.where((quad == 1) | (quad == 2), -c, c)
    s = jnp.where((quad == 2) | (quad == 3), -s, s)
    c, s = jnp.where(used, c, 0.0), jnp.where(used, s, 0.0)
    return jnp.concatenate([jnp.where(imag, s, c), jnp.where(imag, c, -s)], axis=0)


def lines_kernel(
    coef, cols, occ_ref, out_ref,
    lanes, given, got, give_s, got_r,
):
    band, me = lax.axis_index("band"), lax.axis_index("fft")
    yh, zc, c = band // 16, (band // 2) % 8, band % 2
    x, y = me // 2, 2 * yh + me % 2
    slot = 4 * me + 2 * yh + c

    def device(xx, yy, cc):
        return {"band": (yy // 2) * 16 + zc * 2 + cc, "fft": 2 * xx + yy % 2}

    targets = [((x + dx) % 4, (y + dy) % 4, (c + dc) % 2) for dx, dy, dc in TARGETS]
    barrier = pltpu.get_barrier_semaphore()
    for target in targets:
        pl.semaphore_signal(barrier, inc=1, device_id=device(*target), device_id_type=MESH)

    window = cols[pl.ds(pl.multiple_of(640 * me, 128), 704)].reshape(1, 704)
    window = jnp.concatenate([window, window[:, 0:64]], axis=1)
    box = pltpu.roll(window, lax.rem(768 - 8 * me, 768), 1)[:, 0:LC].astype(F32)
    k0 = jnp.floor((box + 0.5) * (1.0 / KZ))
    k1 = box - KZ * k0 - R
    k0 = k0 - R
    k = lax.broadcasted_iota(jnp.int32, (KZ, LC), 0).astype(F32) - R
    inside = k * k + (k0 * k0 + k1 * k1) <= float(R * R)
    scale = jnp.sqrt(jnp.full((1, LC), occ_ref[0].astype(F32) * (1.0 / 32.0)))
    scale = jnp.where(inside, scale, 0.0)
    xt = jnp.concatenate([coef[0, 0] * scale, coef[0, 1] * scale], axis=0).T
    hi, lo = split(xt)
    wh, wl = split(line_table())
    value = dot(hi, wh) + dot(lo, wh) + dot(hi, wl)
    for t in range(3):
        lanes[t] = value[:, 128 * t : 128 * (t + 1)]
    lane = lax.broadcasted_iota(jnp.int32, (56, 128), 1)
    pieces = [(q, 56 if q < 11 else 32) for q in range(12)]

    group = jnp.zeros((56, 128), jnp.int32)
    for q in range(1, 12):
        group = group + (lane >= 10 * q).astype(jnp.int32)
    mine = 2 * yh + c

    def packed(d):
        t, e = d // 12, d % 12
        tile = lanes.at[t]
        result = None
        for q, n in pieces:
            m = lax.rem(q + mine, 12)
            turned = pltpu.roll(tile[56 * q : 56 * q + n, :], lax.rem(1280 + 10 * m - 10 * e, 128), 1)
            if n < 56:
                turned = jnp.concatenate([turned, jnp.zeros((56 - n, 128), F32)], axis=0)
            result = turned if result is None else jnp.where(group == m, turned, result)
        return result

    moves = {}
    for i, target in enumerate(targets):
        xx, yy, cc = target
        given[i] = packed(4 * (2 * xx + yy % 2) + 2 * (yy // 2) + cc)
        if i == 0:
            pl.semaphore_wait(barrier, len(targets))
        move = pltpu.make_async_remote_copy(
            src_ref=given.at[i], dst_ref=got.at[slot],
            send_sem=give_s.at[i], recv_sem=got_r.at[i], device_id=device(*target), device_id_type=MESH,
        )
        move.start()
        moves[TARGETS[i]] = move
    got[slot] = packed(slot)

    def unpack(f):
        base = pl.multiple_of(f * LC, 8)
        for q, n in pieces:
            blocks = [got[4 * f + i, 0:n, :] for i in range(4)]
            here = lane[0:n]
            straight = min(4, 12 - q)
            first = blocks[0]
            for i in range(1, straight):
                first = jnp.where(here >= 10 * (q + i), blocks[i], first)
            result = pltpu.roll(first, 128 - 10 * q, 1) if q else first
            if straight < 4:
                second = blocks[straight]
                for i in range(straight + 1, 4):
                    second = jnp.where(here >= 10 * (q + i - 12), blocks[i], second)
                second = pltpu.roll(second, 120 - 10 * q, 1) if q < 12 else second
                result = jnp.where(here >= 10 * straight, second, result)
            out_ref[pl.ds(base + 56 * q, n), :] = result

    for dx, odd in GROUPS:
        for dy in (odd + 2, odd):
            for dc in (1, 0):
                if (dx, dy, dc) in moves:
                    moves[dx, dy, dc].wait_recv()
        unpack(((x + 4 - dx) % 4) * 2 + (y + odd) % 2)
    for move in moves.values():
        move.wait_send()


def lines(coefficients, cols, occ):
    vmem = pl.BlockSpec(memory_space=pltpu.VMEM)
    dma = pltpu.SemaphoreType.DMA
    n = len(TARGETS)
    return pl.pallas_call(
        lines_kernel,
        out_shape=jax.ShapeDtypeStruct((NCOLS, 128), F32),
        in_specs=[vmem, vmem, pl.BlockSpec(memory_space=pltpu.SMEM)],
        out_specs=vmem,
        scratch_shapes=[
            pltpu.VMEM((3, LC, 128), F32),
            pltpu.VMEM((n, 56, 128), F32),
            pltpu.VMEM((32, 56, 128), F32),
            dma((n,)), dma((n,)),
        ],
        compiler_params=pltpu.CompilerParams(
            collective_id=1, has_side_effects=True, vmem_limit_bytes=LINES_VMEM
        ),
    )(coefficients, cols, occ)


def grid_kernel(rows_ref, cols_ref, out_ref, grid_ref):
    for n in range(NCOLS):
        grid_ref[pl.ds(cols_ref[n], 1), :] = rows_ref[pl.ds(n, 1), :]

    def turn(i, carry):
        for u in range(72):
            k0 = i * 72 + u
            t = grid_ref[pl.ds(pl.multiple_of(k0 * KZ, 8), KZ), :].T[0:40]
            out_ref[pl.ds(k0, 40, stride=KZ), :] = jnp.concatenate([t, jnp.zeros((40, 128 - KZ), F32)], axis=1)
        return carry

    lax.fori_loop(0, KZ // 72, turn, 0)


def grid(rows, cols):
    vmem = pl.BlockSpec(memory_space=pltpu.VMEM)
    return pl.pallas_call(
        grid_kernel,
        out_shape=jax.ShapeDtypeStruct((40 * KZ, 128), F32),
        in_specs=[vmem, pl.BlockSpec(memory_space=pltpu.SMEM)],
        out_specs=vmem,
        scratch_shapes=[pltpu.VMEM((NCOLS + 56, 128), F32)],
        compiler_params=pltpu.CompilerParams(vmem_limit_bytes=GRID_VMEM),
    )(rows, cols)


RELAY = (0,)


def density_kernel(
    g_ref, ch_ref, cl_ref, sh_ref, sl_ref, t2_ref, m3_ref, mh_ref, ml_ref, out_ref,
    hall_ref, part, held, sent, acc, left, fine, packed, given, got,
    ring_s, ring_r, got_s, got_r,
):
    band, me = lax.axis_index("band"), lax.axis_index("fft")
    yh, zc, c = band // 16, (band // 2) % 8, band % 2
    x, y = me // 2, 2 * yh + me % 2
    slot = 4 * me + 2 * yh + c

    def device(xx, yy, cc):
        return {"band": (yy // 2) * 16 + zc * 2 + cc, "fft": 2 * xx + yy % 2}

    ring_to = [{"band": yh * 16 + ((zc + d) % 8) * 2 + c, "fft": me} for d in (6, 7, 1, 2)]
    targets = [((x + dx) % 4, (y + dy) % 4, (c + dc) % 2) for dx, dy, dc in TARGETS]
    barrier = pltpu.get_barrier_semaphore()
    for where in [*ring_to, *(device(*target) for target in targets)]:
        pl.semaphore_signal(barrier, inc=1, device_id=where, device_id_type=MESH)

    started = []

    def copy(src, dst, send, recv, where):
        made = pltpu.make_async_remote_copy(
            src_ref=src, dst_ref=dst, send_sem=send, recv_sem=recv, device_id=where, device_id_type=MESH
        )
        made.start()
        started.append(made)
        return made

    ch, cl, sh, sl = ch_ref[...], cl_ref[...], sh_ref[...], sl_ref[...]
    for h in range(4):
        hall_ref[:, HALF * h + 5 * NC : HALF * (h + 1)] = jnp.zeros((NC, HALF - 5 * NC), F32)

    def first_transform(start, count):
        rows = count * KZ
        for h in range(4):
            base = (10 * h + start) * KZ
            re_h, re_l = split(g_ref[base : base + rows, 0:KZ])
            base += 5 * KZ
            im_h, im_l = split(g_ref[base : base + rows, 0:KZ])
            half_re = (dot(re_h, ch) + dot(re_l, ch) + dot(re_h, cl)) - (
                dot(im_h, sh) + dot(im_l, sh) + dot(im_h, sl)
            )
            half_im = (dot(re_h, sh) + dot(re_l, sh) + dot(re_h, sl)) + (
                dot(im_h, ch) + dot(im_l, ch) + dot(im_h, cl)
            )
            for u in range(count):
                at = HALF * h + NC * (start + u)
                hall_ref[0:KZ, at : at + NC] = half_re[KZ * u : KZ * (u + 1)]
                hall_ref[KZ : 2 * KZ, at : at + NC] = half_im[KZ * u : KZ * (u + 1)]

    row = lax.broadcasted_iota(jnp.int32, (8, 128), 0)

    def chunk(t):
        first_transform(2 * t, min(2, 5 - 2 * t))
        total = 0.0
        for h in range(4):
            hh, hl = split(hall_ref[:, HALF * h + 256 * t : HALF * h + 256 * (t + 1)])
            psi = dot(t2_ref[...], jnp.concatenate([hh, hl, hh], axis=0))
            re, im = psi[0:NC], psi[NC : 2 * NC]
            total = total + (re * re + im * im)
        dh, dl = split(total)
        both = dot(m3_ref[...], jnp.concatenate([dh, dl, dh], axis=0))
        first, second = both[:, 0:128].reshape(8, 5, 8, 128), both[:, 128:256].reshape(8, 5, 8, 128)
        for p in range(4):
            part[:, t, 2 * p] = first[:, p]
            part[:, t, 2 * p + 1] = second[:, p]
        part[:, t, 8] = jnp.where(row[None] < 4, first[:, 4], second[:, 4])

    alone = (pl.ds(0, 4), pl.ds(4, 5))
    ring = {}

    def owner(way, away):
        return (zc + (8 - away if way == 0 else away)) % 8

    def send(way, kind, t, src, units, hops):
        to = {"band": yh * 16 + owner(way, hops) * 2 + c, "fft": me}
        ring[way, kind, t] = copy(
            src, held.at[way, kind, t, units], ring_s.at[way, kind, t], ring_r.at[way, kind, t], to
        )

    def early(t):
        for way in range(2):
            send(way, 0, t, part.at[owner(way, 4), t, alone[way]], alone[way], 2)
        for way in range(2):
            send(way, 1, t, part.at[owner(way, 3), t], pl.ds(0, 9), 1)

    def near(t):
        for way in range(2):
            send(way, 2, t, part.at[owner(way, 1), t], pl.ds(0, 9), 1)

    def joined(t):
        for way in range(2):
            ring[way, 0, t].wait_recv()
            ring[way, 1, t].wait_recv()
            mine, rest = alone[way], alone[1 - way]
            sent[way, 3, t, rest] = part[owner(way, 2), t, rest] + held[way, 1, t, rest]
            sent[way, 3, t, mine] = part[owner(way, 2), t, mine] + held[way, 1, t, mine] + held[way, 0, t, mine]
            send(way, 3, t, sent.at[way, 3, t], pl.ds(0, 9), 2)

    def hop(step, t):
        for way in range(2):
            src, units = part.at[owner(way, 4 - step), t], pl.ds(0, 9)
            if step == 0:
                src, units = part.at[owner(way, 4), t, alone[way]], alone[way]
            else:
                ring[way, step - 1, t].wait_recv()
                mine, rest = alone[way], alone[1 - way]
                here = owner(way, 4 - step)
                if step == 1:
                    sent[way, 1, t, rest] = part[here, t, rest]
                    sent[way, 1, t, mine] = part[here, t, mine] + held[way, 0, t, mine]
                else:
                    sent[way, step, t] = part[here, t] + held[way, step - 1, t]
                src = sent.at[way, step, t]
            send(way, step, t, src, units, 1)

    def final(t):
        for way in range(2):
            if t not in RELAY:
                ring[way, 2, t].wait_recv()
            ring[way, 3, t].wait_recv()
        value = part[zc, t] + held[0, 3, t] + held[1, 3, t]
        if t not in RELAY:
            value = value + held[0, 2, t] + held[1, 2, t]
        acc[t] = value

    chunk(0)
    pl.semaphore_wait(barrier, len(targets) + 4)
    hop(0, 0)
    chunk(1)
    early(1)
    hop(1, 0)
    chunk(2)
    early(2)
    hop(2, 0)
    near(1)
    joined(1)
    near(2)
    hop(3, 0)
    joined(2)
    for t in (1, 0, 2):
        final(t)

    for o in range(4):
        main = jnp.concatenate([acc[t, 2 * o + i] for t in range(3) for i in range(2)], axis=1)
        ninth = jnp.concatenate(
            [acc[t, 8, 4 * i + o : 4 * i + o + 1, :] for t in range(3) for i in range(2)], axis=1
        )
        for u in range(5):
            n = 5 * o + u
            left[8 * n : 8 * n + 8, :] = main[:, NC * u : NC * (u + 1)]
            left[160 + n : 161 + n, :] = ninth[:, NC * u : NC * (u + 1)]
    lh, ll = split(left[...])
    mh, ml = mh_ref[...], ml_ref[...]
    value = dot(lh, mh) + dot(ll, mh) + dot(lh, ml)
    for t in range(3):
        fine[t, :, 0 : min(128, NF - 128 * t)] = value[:, 128 * t : min(128 * (t + 1), NF)]
    for o in range(4):
        for g in range(9):
            here = pl.ds(40 * o + g, 5, stride=8) if g < 8 else pl.ds(160 + 5 * o, 5)
            line = jnp.concatenate([fine[t, here, :] for t in range(3)], axis=1)
            for j in range(8):
                packed[j, o, 0:5, 36 * g : 36 * g + 36] = line[:, 36 * j : 36 * j + 36]
    for j in range(8):
        for o in range(4):
            for t in range(3):
                given[4 * j + o, 5 * t : 5 * t + 5, :] = packed[j, o, 0:5, 128 * t : 128 * (t + 1)]
    moves = []
    farthest = sorted(range(len(targets)), key=lambda i: -sum(min(v, 4 - v) for v in TARGETS[i][:2]))
    for i in farthest:
        xx, yy, cc = targets[i]
        target = targets[i]
        to = 4 * (2 * xx + yy % 2) + 2 * (yy // 2) + cc
        moves.append(copy(given.at[to], got.at[slot], got_s.at[i], got_r.at[i], device(*target)))
    got[slot] = given[slot]
    for one in moves:
        one.wait_recv()
    for j in range(8):
        for o in range(4):
            z = NP * j + FIRST[o]
            for t in range(3):
                out_ref[z : z + COUNT[o], 128 * t : 128 * (t + 1)] = got[4 * j + o, 5 * t : 5 * t + COUNT[o], :]
    for one in started:
        one.wait_send()


def density(g):
    ch, cl, sh, sl = second_tables()
    mh, ml = hi_lo(interpolation().T)
    tables = (ch, cl, sh, sl, first_table(), owner_rows(), mh, ml)
    vmem = pl.BlockSpec(memory_space=pltpu.VMEM)
    dma = pltpu.SemaphoreType.DMA
    n = len(TARGETS)
    return pl.pallas_call(
        density_kernel,
        out_shape=jax.ShapeDtypeStruct((NC, 384), F32),
        in_specs=[vmem] * 9,
        out_specs=vmem,
        scratch_shapes=[
            pltpu.VMEM((NC, 4 * HALF), F32),
            pltpu.VMEM((8, 3, 9, 8, 128), F32),
            pltpu.VMEM((2, 4, 3, 9, 8, 128), F32),
            pltpu.VMEM((2, 4, 3, 9, 8, 128), F32),
            pltpu.VMEM((3, 9, 8, 128), F32),
            pltpu.VMEM((184, NC), F32),
            pltpu.VMEM((3, 184, 128), F32),
            pltpu.VMEM((8, 4, 8, 384), F32),
            pltpu.VMEM((32, 16, 128), F32),
            pltpu.VMEM((32, 16, 128), F32),
            dma((2, 4, 3)), dma((2, 4, 3)),
            dma((n,)), dma((n,)),
        ],
        compiler_params=pltpu.CompilerParams(
            collective_id=0, has_side_effects=True, vmem_limit_bytes=DENSITY_VMEM
        ),
    )(g, *(jnp.asarray(t) for t in tables))


def third_kernel(turned_ref, mh_ref, ml_ref, out_ref):
    rh, rl = split(turned_ref[...].T)
    mh, ml = mh_ref[...], ml_ref[...]
    value = dot(rh, mh) + dot(rl, mh) + dot(rh, ml)
    for g in range(9):
        out_ref[g] = value[36 * g : 36 * g + 36]


def third(turned):
    mh, ml = hi_lo(interpolation().T)
    vmem = pl.BlockSpec(memory_space=pltpu.VMEM)
    return pl.pallas_call(
        third_kernel,
        out_shape=jax.ShapeDtypeStruct((9, 36, NF), F32),
        in_specs=[vmem] * 3,
        out_specs=vmem,
        compiler_params=pltpu.CompilerParams(vmem_limit_bytes=GRID_VMEM),
    )(turned, jnp.asarray(mh), jnp.asarray(ml))


def local(coefficients, col_index, occupation):
    rows = lines(coefficients, col_index, occupation)
    return third(density(grid(rows, col_index)))


def solution(mesh):
    return jax.shard_map(
        local,
        mesh=mesh,
        in_specs=(P("band", None, None, "fft"), P(), P("band")),
        out_specs=P("band", "fft", None),
        check_vma=False,
    )
```
